32 devices in a mesh: grp: 2 (over x), comp: 4 (over z), row: 4 (over y, core).
Axes of the slice: x: 2, y: 2, z: 4, core: 2. Of those that a mesh axis runs over, the one named last changes fastest.
Arguments:
- points: bfloat16 [16384, 1024], P(('grp', 'row')), parts along dimension 0
- mu_init: float32 [2, 2048, 512], P(None, ('grp', 'comp')), parts along dimension 1
- logpi_init: float32 [2, 2048], P(None, ('grp', 'comp')), parts along dimension 1
- inv_temp: float32 [3], replicated
Outputs:
- output 1: float32 [2, 2048, 512], P(None, ('grp', 'comp')), parts along dimension 1
- output 2: float32 [2, 2048], P(None, ('grp', 'comp')), parts along dimension 1
- output 3: float32 [2, 16384], P(None, ('grp', 'row')), parts along dimension 1
There are 2 independent parts. The reference program is written for one: setup_inputs(seed, part) draws one part's arguments, and reference() takes and returns one part's arrays. A program takes and returns all parts, laid end to end along the dimension named above; an argument that names none is the same for every part.
All inputs are finite; a program needn't handle non-finite values.
Results may differ from the reference program's by a relative error of at most 0.001.
Values are sent between devices in bfloat16 or wider.
A program may use at most 1 GiB of HBM per device.

```python
import jax
import jax.numpy as jnp
from jax import lax

POINTS = 8192
DIM = 1024
HALF = 512
COMPS = 1024
SWEEPS = 3
CLUSTERS = 16
BLOCK = 256

EPS_COUNT = 1e-6
PRIOR_ALPHA = 1e-3


def setup_inputs(seed: int = 0, part: int = 0) -> dict:
    base_key = jax.random.key(seed)
    part_key = jax.random.fold_in(base_key, part)
    key_c, key_x, key_j, key_m, key_w = jax.random.split(part_key, 5)
    key_b = jax.random.fold_in(base_key, 1000)
    centers = jax.random.normal(key_c, (2, CLUSTERS, HALF), jnp.float32)
    source = (jnp.arange(POINTS) * CLUSTERS) // POINTS
    noise_x = jax.random.normal(key_x, (2, POINTS, HALF), jnp.float32)
    pts_pair = centers[:, source, :] + 0.7 * noise_x
    points = jnp.transpose(pts_pair, (1, 0, 2)).reshape(POINTS, DIM).astype(jnp.bfloat16)
    pick_ids = jax.random.randint(key_j, (2, COMPS), 0, CLUSTERS)
    noise_m = jax.random.normal(key_m, (2, COMPS, HALF), jnp.float32)
    mu_init = centers[jnp.arange(2)[:, None], pick_ids] + 0.5 * noise_m
    raw_logit = jax.random.normal(key_w, (2, COMPS), jnp.float32)
    logpi_init = raw_logit - jax.nn.logsumexp(raw_logit, axis=1, keepdims=True)
    inv_temp = (0.5 + 1.5 * jax.random.uniform(key_b, (SWEEPS,), jnp.float32)) / HALF
    return {"points": points, "mu_init": mu_init, "logpi_init": logpi_init, "inv_temp": inv_temp}


def reference(points, mu_init, logpi_init, inv_temp):
    x_blocks = points.astype(jnp.float32).reshape(POINTS // BLOCK, BLOCK, 2, HALF)
    x_blocks = jnp.transpose(x_blocks, (0, 2, 1, 3))
    sq_blocks = jnp.sum(x_blocks * x_blocks, axis=3)

    def one_sweep(carry_in, beta_t):
        mean_vecs, log_wts = carry_in
        mu_round = mean_vecs.astype(jnp.bfloat16).astype(jnp.float32)
        mu_sq = jnp.sum(mean_vecs * mean_vecs, axis=2)

        def point_block(acc_pair, block_in):
            x_block, sq_norm = block_in
            cross_dot = jnp.einsum("snh,skh->snk", x_block, mu_round)
            logits = log_wts[:, None, :] - beta_t * (sq_norm[:, :, None] - 2.0 * cross_dot + mu_sq[:, None, :])
            row_max = jnp.max(logits, axis=2)
            shifted = jnp.exp(logits - row_max[:, :, None])
            row_sum = jnp.sum(shifted, axis=2)
            resp_f = shifted / row_sum[:, :, None]
            log_norm = row_max + jnp.log(row_sum)
            resp_round = resp_f.astype(jnp.bfloat16).astype(jnp.float32)
            stat_part = jnp.einsum("snk,snh->skh", resp_round, x_block)
            count_acc, stat_acc = acc_pair
            return (count_acc + jnp.sum(resp_f, axis=1), stat_acc + stat_part), log_norm

        zero_acc = (jnp.zeros((2, COMPS), jnp.float32), jnp.zeros((2, COMPS, HALF), jnp.float32))
        (counts, stat_sum), norm_blocks = lax.scan(point_block, zero_acc, (x_blocks, sq_blocks))
        new_means = stat_sum / (counts[:, :, None] + EPS_COUNT)
        new_logw = jnp.log((counts + PRIOR_ALPHA) / (POINTS + COMPS * PRIOR_ALPHA))
        return (new_means, new_logw), norm_blocks

    (mean_vecs, log_wts), norm_all = lax.scan(one_sweep, (mu_init, logpi_init), inv_temp)
    log_norm = jnp.transpose(norm_all[-1], (1, 0, 2)).reshape(2, POINTS)
    return mean_vecs, log_wts, log_norm
```

```python
import functools

import jax
import jax.numpy as jnp
from jax import lax
from jax.experimental import pallas as pl
from jax.experimental.pallas import tpu as pltpu
from jax.sharding import PartitionSpec as P

EPS_COUNT = 1e-6
PRIOR_ALPHA = 1e-3
MESH = pl.DeviceIdType.MESH
LANE_BLOCK = 256
N_CHUNKS = 4


def _col(row):
    n = row.shape[1]
    parts = [
        jnp.transpose(jnp.broadcast_to(row[:, i : i + 128], (128, 128)))
        for i in range(0, n, 128)
    ]
    return parts[0] if len(parts) == 1 else jnp.concatenate(parts, axis=0)


def _lane_sum_row(block):
    n = block.shape[0]
    parts = [
        jnp.sum(jnp.transpose(block[i : i + 128, :]), axis=0, keepdims=True)
        for i in range(0, n, 128)
    ]
    return parts[0] if len(parts) == 1 else jnp.concatenate(parts, axis=1)


def _fold(x):
    acc = x[:, 0:128]
    for i in range(128, x.shape[1], 128):
        acc = acc + x[:, i : i + 128]
    return acc


def em_kernel(
    n_z, n_sweeps, log_denom,
    x_hbm, mu_hbm, lp_ref, beta_ref,
    mu_out, lp_out, lse_out,
    x_v, mu_f, mu_b, p_v, r_v, s_v, s_rx, s_rx_last, n_tx, n_rx, c_tx, c_rx,
    z_tx, z_rx, m_v, sqx_v, lse_v, lse_rx, lp_rx,
    ld_sem, xs_sem, xr_sem, zs_sem, zr_sem, ss_sem, sr_sem, ns_sem, nr_sem,
    as_sem, ar_sem, cs_sem, cr_sem, ls_sem, lr_sem, os_sem, or_sem,
):
    row = lax.axis_index("row")
    zz = lax.axis_index("comp")
    core = lax.rem(row, 2)
    yy = lax.div(row, 2)
    fit = core
    other = 1 - core
    y_peer = {"row": (1 - yy) * 2 + core}
    c_peer = {"row": yy * 2 + (1 - core)}
    z_peers = [{"comp": lax.rem(zz + d, n_z)} for d in range(1, n_z)]

    n_rows = x_v.shape[0]
    own_rows = n_rows // 2
    k_dim, h_dim = mu_f.shape
    k_half = k_dim // 2
    chunk = n_rows // N_CHUNKS
    per_chunk = chunk // LANE_BLOCK
    mine = pl.multiple_of(yy * k_half, k_half)
    theirs = pl.multiple_of((1 - yy) * k_half, k_half)
    own_chunks = N_CHUNKS // 2

    loads = []
    mu_load = pltpu.make_async_copy(mu_hbm.at[fit], mu_f, ld_sem.at[0])
    mu_load.start()
    for i in range(own_chunks):
        cp = pltpu.make_async_copy(
            x_hbm.at[pl.ds(i * chunk, chunk), pl.ds(pl.multiple_of(fit * h_dim, h_dim), h_dim)],
            x_v.at[pl.ds(i * chunk, chunk)],
            ld_sem.at[1 + i],
        )
        cp.start()
        loads.append(cp)

    barrier = pltpu.get_barrier_semaphore()
    for peer in [c_peer, y_peer] + z_peers:
        pl.semaphore_signal(barrier, inc=1, device_id=peer, device_id_type=MESH)
    pl.semaphore_wait(barrier, 1 + n_z)

    swaps = []
    for i in range(own_chunks):
        cp = pltpu.make_async_remote_copy(
            src_ref=x_hbm.at[pl.ds(i * chunk, chunk), pl.ds(pl.multiple_of(other * h_dim, h_dim), h_dim)],
            dst_ref=x_v.at[pl.ds(own_rows + i * chunk, chunk)],
            send_sem=xs_sem.at[i],
            recv_sem=xr_sem.at[i],
            device_id=c_peer,
            device_id_type=MESH,
        )
        cp.start()
        swaps.append(cp)

    mu_load.wait()
    mu0 = mu_f[...]
    mu_b[...] = mu0.astype(jnp.bfloat16)
    lp0 = jnp.where(core == 0, lp_ref[0:1, :], lp_ref[1:2, :])
    c_row = lp0 - beta_ref[0] * _lane_sum_row(_fold(mu0 * mu0))
    c_col = _col(c_row)

    for t in range(n_sweeps):
        last = t == n_sweeps - 1
        beta = beta_ref[t]
        z_copies = []
        for ci in range(N_CHUNKS):
            if t == 0:
                if ci < own_chunks:
                    loads[ci].wait()
                else:
                    swaps[ci - own_chunks].wait_recv()
            for bi in range(per_chunk):
                r0 = ci * chunk + bi * LANE_BLOCK
                a = lax.dot_general(
                    mu_b[...], x_v[r0 : r0 + LANE_BLOCK, :],
                    (((1,), (1,)), ((), ())), preferred_element_type=jnp.float32,
                )
                lg = a * (2.0 * beta) + jnp.concatenate([c_col] * (LANE_BLOCK // 128), axis=1)
                m = jnp.max(lg, axis=0, keepdims=True)
                p = jnp.exp(lg - m)
                l = m + jnp.log(jnp.sum(p, axis=0, keepdims=True))
                p_v[:, r0 : r0 + LANE_BLOCK] = p
                m_v[:, r0 : r0 + LANE_BLOCK] = m
                z_tx[t, ci, :, bi * LANE_BLOCK : (bi + 1) * LANE_BLOCK] = l
            copies = []
            for d, peer in enumerate(z_peers):
                cp = pltpu.make_async_remote_copy(
                    src_ref=z_tx.at[t, ci],
                    dst_ref=z_rx.at[t, ci, d],
                    send_sem=zs_sem.at[t, ci, d],
                    recv_sem=zr_sem.at[t, ci, d],
                    device_id=peer,
                    device_id_type=MESH,
                )
                cp.start()
                copies.append(cp)
            z_copies.append(copies)

        n_acc = jnp.zeros((k_dim, 128), jnp.float32)
        for ci in range(N_CHUNKS):
            for cp in z_copies[ci]:
                cp.wait_recv()
            for bi in range(per_chunk):
                r0 = ci * chunk + bi * LANE_BLOCK
                sl = slice(bi * LANE_BLOCK, (bi + 1) * LANE_BLOCK)
                parts = [z_tx[t, ci, :, sl]] + [z_rx[t, ci, d, :, sl] for d in range(n_z - 1)]
                top = functools.reduce(jnp.maximum, parts)
                tot = functools.reduce(lambda u, v: u + v, [jnp.exp(q - top) for q in parts])
                lse = top + jnp.log(tot)
                scale = jnp.exp(m_v[:, r0 : r0 + LANE_BLOCK] - lse)
                r = p_v[:, r0 : r0 + LANE_BLOCK] * scale
                r_v[:, r0 : r0 + LANE_BLOCK] = r.astype(jnp.bfloat16)
                n_acc = n_acc + _fold(r)
                if last:
                    lse_v[:, r0 : r0 + LANE_BLOCK] = lse - beta * sqx_v[:, r0 : r0 + LANE_BLOCK]
        n_part = _lane_sum_row(n_acc)
        n_tx[t] = n_part
        n_copy = pltpu.make_async_remote_copy(
            src_ref=n_tx.at[t], dst_ref=n_rx.at[t], send_sem=ns_sem.at[t], recv_sem=nr_sem.at[t],
            device_id=y_peer, device_id_type=MESH,
        )
        n_copy.start()

        s_copies = []
        for hi in range(2):
            cols = slice(hi * (h_dim // 2), (hi + 1) * (h_dim // 2))
            s_v[pl.ds(theirs, k_half), cols] = jnp.dot(
                r_v[pl.ds(theirs, k_half), :], x_v[:, cols], preferred_element_type=jnp.float32
            )
            dst = s_rx_last.at[pl.ds(theirs, k_half), cols] if last else s_rx.at[t, :, cols]
            cp = pltpu.make_async_remote_copy(
                src_ref=s_v.at[pl.ds(theirs, k_half), cols], dst_ref=dst,
                send_sem=ss_sem.at[t, hi], recv_sem=sr_sem.at[t, hi],
                device_id=y_peer, device_id_type=MESH,
            )
            cp.start()
            s_copies.append(cp)
        for hi in range(2):
            cols = slice(hi * (h_dim // 2), (hi + 1) * (h_dim // 2))
            s_v[pl.ds(mine, k_half), cols] = jnp.dot(
                r_v[pl.ds(mine, k_half), :], x_v[:, cols], preferred_element_type=jnp.float32
            )
            if last:
                cp = pltpu.make_async_remote_copy(
                    src_ref=s_v.at[pl.ds(mine, k_half), cols],
                    dst_ref=s_rx_last.at[pl.ds(mine, k_half), cols],
                    send_sem=ss_sem.at[t, 2 + hi], recv_sem=sr_sem.at[t, 2 + hi],
                    device_id=y_peer, device_id_type=MESH,
                )
                cp.start()
                s_copies.append(cp)

        if t == 0:
            ones = jnp.ones((16, h_dim), jnp.bfloat16)
            for b in range(n_rows // LANE_BLOCK):
                r0 = b * LANE_BLOCK
                xf = x_v[r0 : r0 + LANE_BLOCK, :].astype(jnp.float32)
                sq = xf * xf
                hi_part = sq.astype(jnp.bfloat16)
                lo_part = (sq - hi_part.astype(jnp.float32)).astype(jnp.bfloat16)
                acc = lax.dot_general(ones, hi_part, (((1,), (1,)), ((), ())), preferred_element_type=jnp.float32)
                acc = acc + lax.dot_general(ones, lo_part, (((1,), (1,)), ((), ())), preferred_element_type=jnp.float32)
                sqx_v[:, r0 : r0 + LANE_BLOCK] = acc[0:1, :]

        if not last:
            n_copy.wait_recv()
            n_all = n_part + n_rx[t]
            n_own = jnp.where(yy == 0, n_all[:, 0:k_half], n_all[:, k_half:])
            inv_col = _col(1.0 / (n_own + EPS_COUNT))
            for cp in s_copies:
                cp.wait_recv()
            sq_acc = jnp.zeros((k_half, 128), jnp.float32)
            for g in range(h_dim // 128):
                cols = slice(g * 128, (g + 1) * 128)
                mu = (s_v[pl.ds(mine, k_half), cols] + s_rx[t, :, cols]) * inv_col
                mu_b[pl.ds(mine, k_half), cols] = mu.astype(jnp.bfloat16)
                sq_acc = sq_acc + mu * mu
            mu_copy = pltpu.make_async_remote_copy(
                src_ref=mu_b.at[pl.ds(mine, k_half)], dst_ref=mu_b.at[pl.ds(mine, k_half)],
                send_sem=as_sem.at[t], recv_sem=ar_sem.at[t], device_id=y_peer, device_id_type=MESH,
            )
            mu_copy.start()
            c_own = jnp.log((n_own + PRIOR_ALPHA) / log_denom) - beta_ref[t + 1] * _lane_sum_row(sq_acc)
            c_tx[t] = c_own
            c_copy = pltpu.make_async_remote_copy(
                src_ref=c_tx.at[t], dst_ref=c_rx.at[t], send_sem=cs_sem.at[t], recv_sem=cr_sem.at[t],
                device_id=y_peer, device_id_type=MESH,
            )
            c_copy.start()
            c_copy.wait_recv()
            c_peer_row = c_rx[t]
            c_row = jnp.concatenate(
                [jnp.where(yy == 0, c_own, c_peer_row), jnp.where(yy == 0, c_peer_row, c_own)], axis=1
            )
            c_col = _col(c_row)
            mu_copy.wait_recv()
            mu_copy.wait_send()
            c_copy.wait_send()
        else:
            lse_copy = pltpu.make_async_remote_copy(
                src_ref=lse_v.at[:, pl.ds(own_rows, own_rows)], dst_ref=lse_rx,
                send_sem=ls_sem.at[0], recv_sem=lr_sem.at[0], device_id=c_peer, device_id_type=MESH,
            )
            lse_copy.start()
            n_copy.wait_recv()
            n_all = n_part + n_rx[t]
            lp_row = jnp.log((n_all + PRIOR_ALPHA) / log_denom)
            n_tx[t + 1] = lp_row
            lp_copy = pltpu.make_async_remote_copy(
                src_ref=n_tx.at[t + 1], dst_ref=lp_rx,
                send_sem=ls_sem.at[1], recv_sem=lr_sem.at[1], device_id=c_peer, device_id_type=MESH,
            )
            lp_copy.start()
            inv_col = _col(1.0 / (n_all + EPS_COUNT))
            out_copies = []
            for i in range(4):
                hi = i % 2
                base = mine if i < 2 else theirs
                s_copies[i].wait_recv()
                inv_half = jnp.where(yy == (0 if i < 2 else 1), inv_col[0:k_half, :], inv_col[k_half:, :])
                for g in range(h_dim // 256):
                    cols = slice(hi * (h_dim // 2) + g * 128, hi * (h_dim // 2) + (g + 1) * 128)
                    mu_out[fit, pl.ds(base, k_half), cols] = (
                        s_v[pl.ds(base, k_half), cols] + s_rx_last[pl.ds(base, k_half), cols]
                    ) * inv_half
                half = slice(hi * (h_dim // 2), (hi + 1) * (h_dim // 2))
                cp = pltpu.make_async_remote_copy(
                    src_ref=mu_out.at[fit, pl.ds(base, k_half), half],
                    dst_ref=mu_out.at[fit, pl.ds(base, k_half), half],
                    send_sem=os_sem.at[i], recv_sem=or_sem.at[i], device_id=c_peer, device_id_type=MESH,
                )
                cp.start()
                out_copies.append(cp)
            lse_copy.wait_recv()
            own_lse = lse_v[:, 0:own_rows]
            lse_out[0:1, :] = jnp.where(core == 0, own_lse, lse_rx[...])
            lse_out[1:2, :] = jnp.where(core == 0, lse_rx[...], own_lse)
            lp_copy.wait_recv()
            lp_out[0:1, :] = jnp.where(core == 0, lp_row, lp_rx[...])
            lp_out[1:2, :] = jnp.where(core == 0, lp_rx[...], lp_row)
            lse_copy.wait_send()
            lp_copy.wait_send()
            for cp in out_copies:
                cp.wait_send()
                cp.wait_recv()
        n_copy.wait_send()
        for cp in s_copies:
            cp.wait_send()
        for copies in z_copies:
            for cp in copies:
                cp.wait_send()
    for cp in swaps:
        cp.wait_send()


def solution(mesh):
    n_z = mesh.shape["comp"]
    row_size = mesh.shape["row"]

    def local_fit(x_local, mu_init, logpi_init, inv_temp):
        n_rows, full_dim = x_local.shape
        _, k_dim, h_dim = mu_init.shape
        n_sweeps = inv_temp.shape[0]
        total = 2 * n_rows
        chunk = total // N_CHUNKS
        k_half = k_dim // 2
        log_denom = float(n_rows * row_size + k_dim * n_z * PRIOR_ALPHA)
        f32 = jnp.float32
        bf16 = jnp.bfloat16
        dma = pltpu.SemaphoreType.DMA
        mu, lp, lse = pl.pallas_call(
            functools.partial(em_kernel, n_z, n_sweeps, log_denom),
            out_shape=(
                jax.ShapeDtypeStruct((2, k_dim, h_dim), f32),
                jax.ShapeDtypeStruct((2, k_dim), f32),
                jax.ShapeDtypeStruct((2, n_rows), f32),
            ),
            in_specs=[
                pl.BlockSpec(memory_space=pl.ANY),
                pl.BlockSpec(memory_space=pl.ANY),
                pl.BlockSpec(memory_space=pltpu.VMEM),
                pl.BlockSpec(memory_space=pltpu.SMEM),
            ],
            out_specs=(
                pl.BlockSpec(memory_space=pltpu.VMEM),
                pl.BlockSpec(memory_space=pltpu.VMEM),
                pl.BlockSpec(memory_space=pltpu.VMEM),
            ),
            scratch_shapes=[
                pltpu.VMEM((total, h_dim), bf16),
                pltpu.VMEM((k_dim, h_dim), f32),
                pltpu.VMEM((k_dim, h_dim), bf16),
                pltpu.VMEM((k_dim, total), f32),
                pltpu.VMEM((k_dim, total), bf16),
                pltpu.VMEM((k_dim, h_dim), f32),
                pltpu.VMEM((n_sweeps - 1, k_half, h_dim), f32),
                pltpu.VMEM((k_dim, h_dim), f32),
                pltpu.VMEM((n_sweeps + 1, 1, k_dim), f32),
                pltpu.VMEM((n_sweeps, 1, k_dim), f32),
                pltpu.VMEM((n_sweeps, 1, k_half), f32),
                pltpu.VMEM((n_sweeps, 1, k_half), f32),
                pltpu.VMEM((n_sweeps, N_CHUNKS, 1, chunk), f32),
                pltpu.VMEM((n_sweeps, N_CHUNKS, n_z - 1, 1, chunk), f32),
                pltpu.VMEM((1, total), f32),
                pltpu.VMEM((1, total), f32),
                pltpu.VMEM((1, total), f32),
                pltpu.VMEM((1, n_rows), f32),
                pltpu.VMEM((1, k_dim), f32),
                dma((1 + N_CHUNKS // 2,)),
                dma((N_CHUNKS // 2,)), dma((N_CHUNKS // 2,)),
                dma((n_sweeps, N_CHUNKS, n_z - 1)), dma((n_sweeps, N_CHUNKS, n_z - 1)),
                dma((n_sweeps, 4)), dma((n_sweeps, 4)),
                dma((n_sweeps,)), dma((n_sweeps,)),
                dma((n_sweeps,)), dma((n_sweeps,)),
                dma((n_sweeps,)), dma((n_sweeps,)),
                dma((2,)), dma((2,)),
                dma((4,)), dma((4,)),
            ],
            compiler_params=pltpu.CompilerParams(
                collective_id=0, has_side_effects=True, vmem_limit_bytes=60 * 1024 * 1024
            ),
            name="em_kernel",
        )(x_local, mu_init, logpi_init, inv_temp)
        return mu, lp, lse

    return jax.shard_map(
        local_fit,
        mesh=mesh,
        in_specs=(P(("grp", "row"), None), P(None, ("grp", "comp"), None), P(None, ("grp", "comp")), P()),
        out_specs=(P(None, ("grp", "comp"), None), P(None, ("grp", "comp")), P(None, ("grp", "row"))),
        check_vma=False,
    )
```

```python
import functools

import jax
import jax.numpy as jnp
from jax import lax
from jax.experimental import pallas as pl
from jax.experimental.pallas import tpu as pltpu
from jax.sharding import PartitionSpec as P

EPS_COUNT = 1e-6
PRIOR_ALPHA = 1e-3
MESH = pl.DeviceIdType.MESH
LANE_BLOCK = 512
N_CHUNKS = 4
VMEM_LIMIT = 40 * 1024 * 1024


def _col(row):
    n = row.shape[1]
    parts = [
        jnp.transpose(jnp.broadcast_to(row[:, i : i + 128], (128, 128)))
        for i in range(0, n, 128)
    ]
    return parts[0] if len(parts) == 1 else jnp.concatenate(parts, axis=0)


def _lane_sum_row(block):
    n = block.shape[0]
    parts = [
        jnp.sum(jnp.transpose(block[i : i + 128, :]), axis=0, keepdims=True)
        for i in range(0, n, 128)
    ]
    return parts[0] if len(parts) == 1 else jnp.concatenate(parts, axis=1)


def _fold(x):
    acc = x[:, 0:128]
    for i in range(128, x.shape[1], 128):
        acc = acc + x[:, i : i + 128]
    return acc


def em_kernel(
    n_z, n_sweeps, log_denom,
    x_hbm, mu_hbm, lp_hbm, beta_hbm,
    mu_out, lp_out, lse_out,
    x_v, mu_f, mu_b, p_v, r_v, s_v, s_rx, s_rx_last, n_tx, n_rx, c_tx, c_rx,
    z_tx, z_rx, m_v, sqx_v, lse_v, lse_rx, lp_rx, lp_v, beta_ref,
    ld_sem, xs_sem, xr_sem, zs_sem, zr_sem, ss_sem, sr_sem, ns_sem, nr_sem,
    as_sem, ar_sem, cs_sem, cr_sem, ls_sem, lr_sem, os_sem, or_sem, turn_sem,
):
    row = lax.axis_index("row")
    zz = lax.axis_index("comp")
    core = lax.rem(row, 2)
    yy = lax.div(row, 2)
    fit = core
    other = 1 - core
    y_peer = {"row": (1 - yy) * 2 + core}
    c_peer = {"row": yy * 2 + (1 - core)}
    z_peers = [{"comp": lax.rem(zz + d, n_z)} for d in range(1, n_z)]

    n_rows = x_v.shape[0]
    own_rows = n_rows // 2
    k_dim, h_dim = mu_f.shape
    k_half = k_dim // 2
    chunk = n_rows // N_CHUNKS
    per_chunk = chunk // LANE_BLOCK
    mine = pl.multiple_of(yy * k_half, k_half)
    theirs = pl.multiple_of((1 - yy) * k_half, k_half)
    own_chunks = N_CHUNKS // 2
    col_blocks = [slice(g * 128, (g + 1) * 128) for g in range(h_dim // 128)]

    barrier = pltpu.get_barrier_semaphore()
    for peer in [c_peer, y_peer] + z_peers:
        pl.semaphore_signal(barrier, inc=1, device_id=peer, device_id_type=MESH)

    beta_load = pltpu.make_async_copy(beta_hbm, beta_ref, ld_sem.at[0])
    lp_load = pltpu.make_async_copy(lp_hbm, lp_v, ld_sem.at[1])
    mu_load = pltpu.make_async_copy(mu_hbm.at[fit], mu_f, ld_sem.at[2])
    for cp in (beta_load, lp_load, mu_load):
        cp.start()
    loads = []
    for i in range(own_chunks):
        cp = pltpu.make_async_copy(
            x_hbm.at[pl.ds(i * chunk, chunk), pl.ds(pl.multiple_of(fit * h_dim, h_dim), h_dim)],
            x_v.at[pl.ds(i * chunk, chunk)],
            ld_sem.at[3 + i],
        )
        cp.start()
        loads.append(cp)

    with jax.named_scope("enter"):
        pl.semaphore_wait(barrier, 1 + n_z)

    swaps = []
    for i in range(own_chunks):
        cp = pltpu.make_async_remote_copy(
            src_ref=x_hbm.at[pl.ds(i * chunk, chunk), pl.ds(pl.multiple_of(other * h_dim, h_dim), h_dim)],
            dst_ref=x_v.at[pl.ds(own_rows + i * chunk, chunk)],
            send_sem=xs_sem.at[i],
            recv_sem=xr_sem.at[i],
            device_id=c_peer,
            device_id_type=MESH,
        )
        cp.start()
        swaps.append(cp)

    with jax.named_scope("init"):
        beta_load.wait()
        lp_load.wait()
        mu_load.wait()
        mu0 = mu_f[...]
        mu_b[...] = mu0.astype(jnp.bfloat16)
        lp0 = jnp.where(core == 0, lp_v[0:1, :], lp_v[1:2, :])
        c_row = lp0 - beta_ref[0] * _lane_sum_row(_fold(mu0 * mu0))
        c_col = _col(c_row)

    mu_copies = []
    for t in range(n_sweeps):
        last = t == n_sweeps - 1
        beta = beta_ref[t]
        z_copies = []
        for ci in range(N_CHUNKS):
            if t == 0:
                with jax.named_scope("xwait"):
                    if ci < own_chunks:
                        loads[ci].wait()
                    else:
                        swaps[ci - own_chunks].wait_recv()
            with jax.named_scope("estep"):
                for bi in range(per_chunk):
                    r0 = ci * chunk + bi * LANE_BLOCK
                    a = lax.dot_general(
                        mu_b[...], x_v[r0 : r0 + LANE_BLOCK, :],
                        (((1,), (1,)), ((), ())), preferred_element_type=jnp.float32,
                    )
                    lg = a * (2.0 * beta) + jnp.concatenate([c_col] * (LANE_BLOCK // 128), axis=1)
                    m = jnp.max(lg, axis=0, keepdims=True)
                    p = jnp.exp(lg - m)
                    l = m + jnp.log(jnp.sum(p, axis=0, keepdims=True))
                    p_v[:, r0 : r0 + LANE_BLOCK] = p
                    m_v[:, r0 : r0 + LANE_BLOCK] = m
                    z_tx[t, ci, :, bi * LANE_BLOCK : (bi + 1) * LANE_BLOCK] = l
            copies = []
            for d, peer in enumerate(z_peers):
                cp = pltpu.make_async_remote_copy(
                    src_ref=z_tx.at[t, ci],
                    dst_ref=z_rx.at[t, ci, d],
                    send_sem=zs_sem.at[t, ci, d],
                    recv_sem=zr_sem.at[t, ci, d],
                    device_id=peer,
                    device_id_type=MESH,
                )
                cp.start()
                copies.append(cp)
            z_copies.append(copies)

        n_acc = jnp.zeros((k_dim, 128), jnp.float32)
        for ci in range(N_CHUNKS):
            with jax.named_scope("zwait"):
                for cp in z_copies[ci]:
                    cp.wait_recv()
            with jax.named_scope("resp"):
                for bi in range(per_chunk):
                    r0 = ci * chunk + bi * LANE_BLOCK
                    sl = slice(bi * LANE_BLOCK, (bi + 1) * LANE_BLOCK)
                    parts = [z_tx[t, ci, :, sl]] + [z_rx[t, ci, d, :, sl] for d in range(n_z - 1)]
                    top = functools.reduce(jnp.maximum, parts)
                    tot = functools.reduce(lambda u, v: u + v, [jnp.exp(q - top) for q in parts])
                    lse = top + jnp.log(tot)
                    scale = jnp.exp(m_v[:, r0 : r0 + LANE_BLOCK] - lse)
                    r = p_v[:, r0 : r0 + LANE_BLOCK] * scale
                    r_v[:, r0 : r0 + LANE_BLOCK] = r.astype(jnp.bfloat16)
                    n_acc = n_acc + _fold(r)
                    if last:
                        lse_v[:, r0 : r0 + LANE_BLOCK] = lse - beta * sqx_v[:, r0 : r0 + LANE_BLOCK]
                rows = slice(ci * chunk, (ci + 1) * chunk)
                part = jnp.dot(
                    r_v[pl.ds(theirs, k_half), rows], x_v[rows, :], preferred_element_type=jnp.float32
                )
                s_v[pl.ds(theirs, k_half), :] = part if ci == 0 else s_v[pl.ds(theirs, k_half), :] + part

        n_part = _lane_sum_row(n_acc)
        n_tx[t] = n_part
        n_copy = pltpu.make_async_remote_copy(
            src_ref=n_tx.at[t], dst_ref=n_rx.at[t], send_sem=ns_sem.at[t], recv_sem=nr_sem.at[t],
            device_id=y_peer, device_id_type=MESH,
        )
        n_copy.start()
        if t == 0:
            with jax.named_scope("turn"):
                @pl.when(core == 0)
                def _():
                    pl.semaphore_wait(turn_sem, 1)
        s_copies = []

        def send_s(half, g, slot):
            dst = s_rx_last.at[pl.ds(half, k_half), col_blocks[g]] if last else s_rx.at[t, :, col_blocks[g]]
            cp = pltpu.make_async_remote_copy(
                src_ref=s_v.at[pl.ds(half, k_half), col_blocks[g]], dst_ref=dst,
                send_sem=ss_sem.at[t, slot], recv_sem=sr_sem.at[t, slot],
                device_id=y_peer, device_id_type=MESH,
            )
            cp.start()
            s_copies.append(cp)

        for g in range(len(col_blocks)):
            send_s(theirs, g, g)
        with jax.named_scope("smine"):
            s_v[pl.ds(mine, k_half), :] = jnp.dot(
                r_v[pl.ds(mine, k_half), :], x_v[...], preferred_element_type=jnp.float32
            )
        if last:
            for g in range(len(col_blocks)):
                send_s(mine, g, len(col_blocks) + g)

        if t == 0:
            with jax.named_scope("pass"):
                for cp in s_copies:
                    cp.wait_send()
                @pl.when(core == 1)
                def _():
                    pl.semaphore_signal(turn_sem, inc=1, device_id=c_peer, device_id_type=MESH)
            with jax.named_scope("sqx"):
                ones = jnp.ones((16, h_dim), jnp.bfloat16)
                for b in range(n_rows // 512):
                    r0 = b * 512
                    xf = x_v[r0 : r0 + 512, :].astype(jnp.float32)
                    sq = xf * xf
                    hi_part = sq.astype(jnp.bfloat16)
                    lo_part = (sq - hi_part.astype(jnp.float32)).astype(jnp.bfloat16)
                    acc = lax.dot_general(ones, hi_part, (((1,), (1,)), ((), ())), preferred_element_type=jnp.float32)
                    acc = acc + lax.dot_general(ones, lo_part, (((1,), (1,)), ((), ())), preferred_element_type=jnp.float32)
                    sqx_v[:, r0 : r0 + 512] = acc[0:1, :]

        if not last:
            with jax.named_scope("nwait"):
                n_copy.wait_recv()
            n_all = n_part + n_rx[t]
            n_own = jnp.where(yy == 0, n_all[:, 0:k_half], n_all[:, k_half:])
            inv_col = _col(1.0 / (n_own + EPS_COUNT))
            sq_acc = jnp.zeros((k_half, 128), jnp.float32)
            mu_copies = []
            for g, cols in enumerate(col_blocks):
                with jax.named_scope("ywait"):
                    s_copies[g].wait_recv()
                with jax.named_scope("mu"):
                    mu = (s_v[pl.ds(mine, k_half), cols] + s_rx[t, :, cols]) * inv_col
                    mu_b[pl.ds(mine, k_half), cols] = mu.astype(jnp.bfloat16)
                    sq_acc = sq_acc + mu * mu
                cp = pltpu.make_async_remote_copy(
                    src_ref=mu_b.at[pl.ds(mine, k_half), cols], dst_ref=mu_b.at[pl.ds(mine, k_half), cols],
                    send_sem=as_sem.at[t, g], recv_sem=ar_sem.at[t, g], device_id=y_peer, device_id_type=MESH,
                )
                cp.start()
                mu_copies.append(cp)
            c_own = jnp.log((n_own + PRIOR_ALPHA) / log_denom) - beta_ref[t + 1] * _lane_sum_row(sq_acc)
            c_tx[t] = c_own
            c_copy = pltpu.make_async_remote_copy(
                src_ref=c_tx.at[t], dst_ref=c_rx.at[t], send_sem=cs_sem.at[t], recv_sem=cr_sem.at[t],
                device_id=y_peer, device_id_type=MESH,
            )
            c_copy.start()
            with jax.named_scope("cwait"):
                c_copy.wait_recv()
            c_peer_row = c_rx[t]
            c_row = jnp.concatenate(
                [jnp.where(yy == 0, c_own, c_peer_row), jnp.where(yy == 0, c_peer_row, c_own)], axis=1
            )
            c_col = _col(c_row)
            with jax.named_scope("muwait"):
                for cp in mu_copies:
                    cp.wait_recv()
                for cp in mu_copies:
                    cp.wait_send()
                c_copy.wait_send()
        else:
            lse_copy = pltpu.make_async_remote_copy(
                src_ref=lse_v.at[:, pl.ds(own_rows, own_rows)], dst_ref=lse_rx,
                send_sem=ls_sem.at[0], recv_sem=lr_sem.at[0], device_id=c_peer, device_id_type=MESH,
            )
            lse_copy.start()
            n_copy.wait_recv()
            n_all = n_part + n_rx[t]
            lp_row = jnp.log((n_all + PRIOR_ALPHA) / log_denom)
            n_tx[t + 1] = lp_row
            lp_copy = pltpu.make_async_remote_copy(
                src_ref=n_tx.at[t + 1], dst_ref=lp_rx,
                send_sem=ls_sem.at[1], recv_sem=lr_sem.at[1], device_id=c_peer, device_id_type=MESH,
            )
            lp_copy.start()
            inv_col = _col(1.0 / (n_all + EPS_COUNT))
            lse_copy.wait_recv()
            own_lse = lse_v[:, 0:own_rows]
            lse_out[0:1, :] = jnp.where(core == 0, own_lse, lse_rx[...])
            lse_out[1:2, :] = jnp.where(core == 0, lse_rx[...], own_lse)
            lp_copy.wait_recv()
            lp_out[0:1, :] = jnp.where(core == 0, lp_row, lp_rx[...])
            lp_out[1:2, :] = jnp.where(core == 0, lp_rx[...], lp_row)
            out_copies = []
            for half in range(2):
                base = mine if half == 0 else theirs
                inv_half = jnp.where(yy == half, inv_col[0:k_half, :], inv_col[k_half:, :])
                for g, cols in enumerate(col_blocks):
                    slot = half * len(col_blocks) + g
                    with jax.named_scope("fwait"):
                        s_copies[slot].wait_recv()
                    with jax.named_scope("fmu"):
                        mu_out[fit, pl.ds(base, k_half), cols] = (
                            s_v[pl.ds(base, k_half), cols] + s_rx_last[pl.ds(base, k_half), cols]
                        ) * inv_half
                    cp = pltpu.make_async_remote_copy(
                        src_ref=mu_out.at[fit, pl.ds(base, k_half), cols],
                        dst_ref=mu_out.at[fit, pl.ds(base, k_half), cols],
                        send_sem=os_sem.at[slot], recv_sem=or_sem.at[slot], device_id=c_peer, device_id_type=MESH,
                    )
                    cp.start()
                    out_copies.append(cp)
            lse_copy.wait_send()
            lp_copy.wait_send()
            with jax.named_scope("owait"):
                for cp in out_copies:
                    cp.wait_send()
                    cp.wait_recv()
        with jax.named_scope("tail"):
            n_copy.wait_send()
            if t > 0:
                for cp in s_copies:
                    cp.wait_send()
            for copies in z_copies:
                for cp in copies:
                    cp.wait_send()
    for cp in swaps:
        cp.wait_send()


def store_kernel(mu_ref, lp_ref, lse_ref, mu_out, lp_out, lse_out, sems):
    copies = []
    parts = 4
    step = mu_ref.shape[1] // parts
    for s in range(mu_ref.shape[0]):
        for i in range(parts):
            rows = pl.ds(i * step, step)
            copies.append(
                pltpu.make_async_copy(mu_ref.at[s, rows], mu_out.at[s, rows], sems.at[2 + s * parts + i])
            )
    copies.append(pltpu.make_async_copy(lp_ref, lp_out, sems.at[0]))
    copies.append(pltpu.make_async_copy(lse_ref, lse_out, sems.at[1]))
    for cp in copies:
        cp.start()
    for cp in copies:
        cp.wait()


def solution(mesh):
    n_z = mesh.shape["comp"]
    row_size = mesh.shape["row"]

    def local_fit(x_local, mu_init, logpi_init, inv_temp):
        n_rows, full_dim = x_local.shape
        _, k_dim, h_dim = mu_init.shape
        n_sweeps = inv_temp.shape[0]
        total = 2 * n_rows
        chunk = total // N_CHUNKS
        k_half = k_dim // 2
        col_blocks = h_dim // 128
        log_denom = float(n_rows * row_size + k_dim * n_z * PRIOR_ALPHA)
        f32 = jnp.float32
        bf16 = jnp.bfloat16
        dma = pltpu.SemaphoreType.DMA
        mu, lp, lse = pl.pallas_call(
            functools.partial(em_kernel, n_z, n_sweeps, log_denom),
            out_shape=(
                pltpu.VMEM((2, k_dim, h_dim), f32),
                pltpu.VMEM((2, k_dim), f32),
                pltpu.VMEM((2, n_rows), f32),
            ),
            in_specs=[pl.BlockSpec(memory_space=pltpu.HBM)] * 4,
            out_specs=(
                pl.BlockSpec(memory_space=pltpu.VMEM),
                pl.BlockSpec(memory_space=pltpu.VMEM),
                pl.BlockSpec(memory_space=pltpu.VMEM),
            ),
            scratch_shapes=[
                pltpu.VMEM((total, h_dim), bf16),
                pltpu.VMEM((k_dim, h_dim), f32),
                pltpu.VMEM((k_dim, h_dim), bf16),
                pltpu.VMEM((k_dim, total), f32),
                pltpu.VMEM((k_dim, total), bf16),
                pltpu.VMEM((k_dim, h_dim), f32),
                pltpu.VMEM((n_sweeps - 1, k_half, h_dim), f32),
                pltpu.VMEM((k_dim, h_dim), f32),
                pltpu.VMEM((n_sweeps + 1, 1, k_dim), f32),
                pltpu.VMEM((n_sweeps, 1, k_dim), f32),
                pltpu.VMEM((n_sweeps, 1, k_half), f32),
                pltpu.VMEM((n_sweeps, 1, k_half), f32),
                pltpu.VMEM((n_sweeps, N_CHUNKS, 1, chunk), f32),
                pltpu.VMEM((n_sweeps, N_CHUNKS, n_z - 1, 1, chunk), f32),
                pltpu.VMEM((1, total), f32),
                pltpu.VMEM((1, total), f32),
                pltpu.VMEM((1, total), f32),
                pltpu.VMEM((1, n_rows), f32),
                pltpu.VMEM((1, k_dim), f32),
                pltpu.VMEM((2, k_dim), f32),
                pltpu.SMEM((n_sweeps,), f32),
                dma((3 + N_CHUNKS // 2,)),
                dma((N_CHUNKS // 2,)), dma((N_CHUNKS // 2,)),
                dma((n_sweeps, N_CHUNKS, n_z - 1)), dma((n_sweeps, N_CHUNKS, n_z - 1)),
                dma((n_sweeps, 2 * col_blocks)), dma((n_sweeps, 2 * col_blocks)),
                dma((n_sweeps,)), dma((n_sweeps,)),
                dma((n_sweeps, col_blocks)), dma((n_sweeps, col_blocks)),
                dma((n_sweeps,)), dma((n_sweeps,)),
                dma((2,)), dma((2,)),
                dma((2 * col_blocks,)), dma((2 * col_blocks,)),
                pltpu.SemaphoreType.REGULAR,
            ],
            compiler_params=pltpu.CompilerParams(
                collective_id=0, has_side_effects=True, vmem_limit_bytes=VMEM_LIMIT
            ),
            name="em_kernel",
        )(*[pltpu.with_memory_space_constraint(v, pltpu.HBM) for v in (x_local, mu_init, logpi_init, inv_temp)])
        return pl.pallas_call(
            store_kernel,
            out_shape=(
                jax.ShapeDtypeStruct((2, k_dim, h_dim), f32),
                jax.ShapeDtypeStruct((2, k_dim), f32),
                jax.ShapeDtypeStruct((2, n_rows), f32),
            ),
            in_specs=[pl.BlockSpec(memory_space=pltpu.VMEM)] * 3,
            out_specs=(pl.BlockSpec(memory_space=pl.ANY),) * 3,
            scratch_shapes=[dma((2 + 2 * 4,))],
            compiler_params=pltpu.CompilerParams(vmem_limit_bytes=4 * 1024 * 1024),
            name="store_kernel",
        )(mu, lp, lse)

    return jax.shard_map(
        local_fit,
        mesh=mesh,
        in_specs=(P(("grp", "row"), None), P(None, ("grp", "comp"), None), P(None, ("grp", "comp")), P()),
        out_specs=(P(None, ("grp", "comp"), None), P(None, ("grp", "comp")), P(None, ("grp", "row"))),
        check_vma=False,
    )
```

```python
import functools

import jax
import jax.numpy as jnp
from jax import lax
from jax.experimental import pallas as pl
from jax.experimental.pallas import tpu as pltpu
from jax.sharding import PartitionSpec as P

EPS_COUNT = 1e-6
PRIOR_ALPHA = 1e-3
MESH = pl.DeviceIdType.MESH
LANE_BLOCK = 512
N_CHUNKS = 4
VMEM_LIMIT = 40 * 1024 * 1024


def _col(row):
    n = row.shape[1]
    parts = [
        jnp.transpose(jnp.broadcast_to(row[:, i : i + 128], (128, 128)))
        for i in range(0, n, 128)
    ]
    return parts[0] if len(parts) == 1 else jnp.concatenate(parts, axis=0)


def _lane_sum_row(block):
    n = block.shape[0]
    parts = [
        jnp.sum(jnp.transpose(block[i : i + 128, :]), axis=0, keepdims=True)
        for i in range(0, n, 128)
    ]
    return parts[0] if len(parts) == 1 else jnp.concatenate(parts, axis=1)


def _fold(x):
    acc = x[:, 0:128]
    for i in range(128, x.shape[1], 128):
        acc = acc + x[:, i : i + 128]
    return acc


def em_kernel(
    n_z, n_sweeps, log_denom,
    x_hbm, mu_hbm, lp_hbm, beta_hbm,
    mu_out, lp_out, lse_out,
    x_v, x_t, mu_f, mu_b, p_v, r_v, s_v, s_rx, n_tx, n_rx, c_tx, c_rx,
    z_tx, z_rx, m_v, l_v, sqx_v, lse_v, lse_rx, lp_rx, lp_v, beta_ref,
    ld_sem, xs_sem, xr_sem, zs_sem, zr_sem, ss_sem, sr_sem, ns_sem, nr_sem,
    as_sem, ar_sem, cs_sem, cr_sem, ls_sem, lr_sem, os_sem, or_sem, turn_sem,
):
    row = lax.axis_index("row")
    zz = lax.axis_index("comp")
    core = lax.rem(row, 2)
    yy = lax.div(row, 2)
    fit = core
    other = 1 - core
    y_peer = {"row": (1 - yy) * 2 + core}
    c_peer = {"row": yy * 2 + (1 - core)}
    z_peers = [{"comp": lax.rem(zz + d, n_z)} for d in range(1, n_z)]

    n_rows = x_v.shape[0]
    own_rows = n_rows // 2
    k_dim, h_dim = mu_f.shape
    k_half = k_dim // 2
    chunk = n_rows // N_CHUNKS
    per_chunk = chunk // LANE_BLOCK
    mine = pl.multiple_of(yy * k_half, k_half)
    theirs = pl.multiple_of((1 - yy) * k_half, k_half)
    own_chunks = N_CHUNKS // 2
    n_col = h_dim // 128
    col_blocks = [slice(g * 128, (g + 1) * 128) for g in range(n_col)]
    lanes = LANE_BLOCK // 128

    def remote(src, dst, send, recv, peer):
        return pltpu.make_async_remote_copy(
            src_ref=src, dst_ref=dst, send_sem=send, recv_sem=recv, device_id=peer, device_id_type=MESH
        )

    barrier = pltpu.get_barrier_semaphore()
    for peer in [c_peer, y_peer] + z_peers:
        pl.semaphore_signal(barrier, inc=1, device_id=peer, device_id_type=MESH)

    my_cols = pl.ds(pl.multiple_of(fit * h_dim, h_dim), h_dim)
    your_cols = pl.ds(pl.multiple_of(other * h_dim, h_dim), h_dim)
    beta_load = pltpu.make_async_copy(beta_hbm, beta_ref, ld_sem.at[0])
    lp_load = pltpu.make_async_copy(lp_hbm, lp_v, ld_sem.at[1])
    mu_load = pltpu.make_async_copy(mu_hbm.at[fit], mu_f, ld_sem.at[2])
    for cp in (beta_load, lp_load, mu_load):
        cp.start()
    loads = []
    for i in range(own_chunks):
        rows = pl.ds(i * chunk, chunk)
        cp = pltpu.make_async_copy(x_hbm.at[rows, my_cols], x_v.at[rows], ld_sem.at[3 + i])
        cp.start()
        loads.append(cp)

    with jax.named_scope("enter"):
        pl.semaphore_wait(barrier, 1 + n_z)

    swaps = []
    for i in range(own_chunks):
        cp = remote(
            x_hbm.at[pl.ds(i * chunk, chunk), your_cols], x_v.at[pl.ds(own_rows + i * chunk, chunk)],
            xs_sem.at[0], xr_sem.at[i], c_peer,
        )
        cp.start()
        swaps.append(cp)

    with jax.named_scope("init"):
        beta_load.wait()
        lp_load.wait()
        mu_load.wait()
        mu0 = mu_f[...]
        mu_b[...] = mu0.astype(jnp.bfloat16)
        lp0 = jnp.where(core == 0, lp_v[0:1, :], lp_v[1:2, :])
        c_row = lp0 - beta_ref[0] * _lane_sum_row(_fold(mu0 * mu0))
        c_col = _col(c_row)

    def softmax_half(lg, half, base, cols):
        m = jnp.max(lg, axis=0, keepdims=True)
        p = jnp.exp(lg - m)
        p_v[pl.ds(base, k_half), cols] = p
        m_v[half, :, cols] = m
        return m + jnp.log(jnp.sum(p, axis=0, keepdims=True))

    def log_add(u, v):
        top = jnp.maximum(u, v)
        return top + jnp.log(jnp.exp(u - top) + jnp.exp(v - top))

    def half_logits(base, cc, beta, cols):
        a = jnp.dot(mu_b[pl.ds(base, k_half), :], x_t[:, cols], preferred_element_type=jnp.float32)
        return a * (2.0 * beta) + jnp.concatenate([cc] * lanes, axis=1)

    for t in range(n_sweeps):
        last = t == n_sweeps - 1
        beta = beta_ref[t]
        par = t % 2
        for ci in range(N_CHUNKS):
            if t == 0:
                with jax.named_scope("xwait"):
                    if ci < own_chunks:
                        loads[ci].wait()
                    else:
                        swaps[ci - own_chunks].wait_recv()
            with jax.named_scope("estep"):
                for bi in range(per_chunk):
                    r0 = ci * chunk + bi * LANE_BLOCK
                    cols = slice(r0, r0 + LANE_BLOCK)
                    if t == 0:
                        a = lax.dot_general(
                            mu_b[...], x_v[cols, :], (((1,), (1,)), ((), ())), preferred_element_type=jnp.float32
                        )
                        lg = a * (2.0 * beta) + jnp.concatenate([c_col] * lanes, axis=1)
                        l0 = softmax_half(lg[0:k_half, :], 0, 0, cols)
                        l1 = softmax_half(lg[k_half:, :], 1, k_half, cols)
                    else:
                        l0 = l_v[:, cols]
                        l1 = softmax_half(half_logits(theirs, c_their_col, beta, cols), 1 - yy, theirs, cols)
                    z_tx[par, ci, :, bi * LANE_BLOCK : (bi + 1) * LANE_BLOCK] = log_add(l0, l1)
            for d, peer in enumerate(z_peers):
                remote(z_tx.at[par, ci], z_rx.at[par, ci, d], zs_sem.at[par], zr_sem.at[par, ci], peer).start()

        n_acc = jnp.zeros((k_dim, 128), jnp.float32)
        for ci in range(N_CHUNKS):
            with jax.named_scope("zwait"):
                remote(z_rx.at[par, ci], z_rx.at[par, ci], zs_sem.at[par], zr_sem.at[par, ci], z_peers[0]).wait_recv()
            with jax.named_scope("resp"):
                for bi in range(per_chunk):
                    r0 = ci * chunk + bi * LANE_BLOCK
                    cols = slice(r0, r0 + LANE_BLOCK)
                    sl = slice(bi * LANE_BLOCK, (bi + 1) * LANE_BLOCK)
                    parts = [z_tx[par, ci, :, sl]] + [z_rx[par, ci, d, :, sl] for d in range(n_z - 1)]
                    top = functools.reduce(jnp.maximum, parts)
                    tot = functools.reduce(lambda u, v: u + v, [jnp.exp(q - top) for q in parts])
                    lse = top + jnp.log(tot)
                    halves = []
                    for h in range(2):
                        ks = slice(h * k_half, (h + 1) * k_half)
                        r = p_v[ks, cols] * jnp.exp(m_v[h, :, cols] - lse)
                        r_v[ks, cols] = r.astype(jnp.bfloat16)
                        halves.append(_fold(r))
                    n_acc = n_acc + jnp.concatenate(halves, axis=0)
                    if last:
                        lse_v[:, cols] = lse - beta * sqx_v[:, cols]
                rows = slice(ci * chunk, (ci + 1) * chunk)
                part = jnp.dot(r_v[pl.ds(theirs, k_half), rows], x_v[rows, :], preferred_element_type=jnp.float32)
                s_v[pl.ds(theirs, k_half), :] = part if ci == 0 else s_v[pl.ds(theirs, k_half), :] + part

        n_part = _lane_sum_row(n_acc)
        n_tx[par] = n_part
        n_copy = remote(n_tx.at[par], n_rx.at[par], ns_sem.at[0], nr_sem.at[0], y_peer)
        n_copy.start()

        def s_copy(half, g, slot):
            return remote(
                s_v.at[pl.ds(half, k_half), col_blocks[g]], s_rx.at[pl.ds(half, k_half), col_blocks[g]],
                ss_sem.at[0 if g < n_col - 1 else 1], sr_sem.at[slot], y_peer,
            )

        first_copies = [s_copy(theirs, g, g) for g in range(n_col)]
        s_mine = jax.named_scope("smine")
        early = s_v.at[pl.ds(theirs, k_half), pl.ds(0, h_dim - 128)]
        late = s_v.at[pl.ds(theirs, k_half), pl.ds(h_dim - 128, 128)]
        early_sent = remote(early, early, ss_sem.at[0], sr_sem.at[0], y_peer)
        late_sent = remote(late, late, ss_sem.at[1], sr_sem.at[0], y_peer)

        if t > 0:
            for cp in first_copies:
                cp.start()
        else:
            @pl.when(core == 1)
            def _():
                for cp in first_copies:
                    cp.start()

        with s_mine:
            s_v[pl.ds(mine, k_half), :] = jnp.dot(
                r_v[pl.ds(mine, k_half), :], x_v[...], preferred_element_type=jnp.float32
            )
        last_copies = []
        if last:
            last_copies = [s_copy(mine, g, n_col + g) for g in range(n_col)]
            for cp in last_copies:
                cp.start()

        if t == 0:
            with jax.named_scope("xt"):
                for b in range(n_rows // LANE_BLOCK):
                    rows = slice(b * LANE_BLOCK, (b + 1) * LANE_BLOCK)
                    x_t[:, rows] = jnp.transpose(x_v[rows, :])
            with jax.named_scope("turn"):
                @pl.when(core == 1)
                def _():
                    early_sent.wait_send()
                    pl.semaphore_signal(turn_sem, inc=1, device_id=c_peer, device_id_type=MESH)

                @pl.when(core == 0)
                def _():
                    pl.semaphore_wait(turn_sem, 1)
                    for cp in first_copies:
                        cp.start()
                    early_sent.wait_send()

            with jax.named_scope("sqx"):
                for b in range(n_rows // LANE_BLOCK):
                    cols = slice(b * LANE_BLOCK, (b + 1) * LANE_BLOCK)
                    xf = x_t[:, cols].astype(jnp.float32)
                    sqx_v[:, cols] = jnp.sum(xf * xf, axis=0, keepdims=True)

        with jax.named_scope("nwait"):
            n_copy.wait_recv()
        n_all = n_part + n_rx[par]
        if not last:
            n_own = jnp.where(yy == 0, n_all[:, 0:k_half], n_all[:, k_half:])
            inv_col = _col(1.0 / (n_own + EPS_COUNT))
            sq_acc = jnp.zeros((k_half, 128), jnp.float32)
            for g, cols in enumerate(col_blocks):
                with jax.named_scope("ywait"):
                    first_copies[g].wait_recv()
                with jax.named_scope("mu"):
                    mu = (s_v[pl.ds(mine, k_half), cols] + s_rx[pl.ds(mine, k_half), cols]) * inv_col
                    mu_b[pl.ds(mine, k_half), cols] = mu.astype(jnp.bfloat16)
                    sq_acc = sq_acc + mu * mu
                block = mu_b.at[pl.ds(mine, k_half), cols]
                remote(block, block, as_sem.at[0], ar_sem.at[0], y_peer).start()
            c_own = jnp.log((n_own + PRIOR_ALPHA) / log_denom) - beta_ref[t + 1] * _lane_sum_row(sq_acc)
            c_tx[par] = c_own
            c_copy = remote(c_tx.at[par], c_rx.at[par], cs_sem.at[0], cr_sem.at[0], y_peer)
            c_copy.start()
            c_own_col = _col(c_own)
            with jax.named_scope("emine"):
                for b in range(n_rows // LANE_BLOCK):
                    cols = slice(b * LANE_BLOCK, (b + 1) * LANE_BLOCK)
                    l_v[:, cols] = softmax_half(
                        half_logits(mine, c_own_col, beta_ref[t + 1], cols), yy, mine, cols
                    )
            with jax.named_scope("cwait"):
                c_copy.wait_recv()
                c_their_col = _col(c_rx[par])
            with jax.named_scope("muwait"):
                sent, came = mu_b.at[pl.ds(mine, k_half)], mu_b.at[pl.ds(theirs, k_half)]
                remote(sent, came, as_sem.at[0], ar_sem.at[0], y_peer).wait()
                c_copy.wait_send()
        else:
            lse_copy = remote(lse_v.at[:, pl.ds(own_rows, own_rows)], lse_rx, ls_sem.at[0], lr_sem.at[0], c_peer)
            lse_copy.start()
            lp_row = jnp.log((n_all + PRIOR_ALPHA) / log_denom)
            n_tx[1 - par] = lp_row
            lp_copy = remote(n_tx.at[1 - par], lp_rx, ls_sem.at[1], lr_sem.at[1], c_peer)
            lp_copy.start()
            inv_col = _col(1.0 / (n_all + EPS_COUNT))
            lse_copy.wait_recv()
            own_lse = lse_v[:, 0:own_rows]
            lse_out[0:1, :] = jnp.where(core == 0, own_lse, lse_rx[...])
            lse_out[1:2, :] = jnp.where(core == 0, lse_rx[...], own_lse)
            lp_copy.wait_recv()
            lp_out[0:1, :] = jnp.where(core == 0, lp_row, lp_rx[...])
            lp_out[1:2, :] = jnp.where(core == 0, lp_rx[...], lp_row)
            for half in range(2):
                base = mine if half == 0 else theirs
                inv_half = jnp.where(yy == half, inv_col[0:k_half, :], inv_col[k_half:, :])
                for g, cols in enumerate(col_blocks):
                    with jax.named_scope("fwait"):
                        (first_copies if half == 0 else last_copies)[g].wait_recv()
                    with jax.named_scope("fmu"):
                        mu_out[fit, pl.ds(base, k_half), cols] = (
                            s_v[pl.ds(base, k_half), cols] + s_rx[pl.ds(base, k_half), cols]
                        ) * inv_half
                    block = mu_out.at[fit, pl.ds(base, k_half), cols]
                    remote(block, block, os_sem.at[0], or_sem.at[0], c_peer).start()
            lse_copy.wait_send()
            lp_copy.wait_send()
            with jax.named_scope("owait"):
                remote(mu_out.at[fit], mu_out.at[fit], os_sem.at[0], or_sem.at[0], c_peer).wait()
        with jax.named_scope("tail"):
            n_copy.wait_send()
            if last:
                both = s_v.at[:, pl.ds(0, h_dim - 128)]
                remote(both, both, ss_sem.at[0], sr_sem.at[0], y_peer).wait_send()
                both = s_v.at[:, pl.ds(h_dim - 128, 128)]
                remote(both, both, ss_sem.at[1], sr_sem.at[0], y_peer).wait_send()
            else:
                if t > 0:
                    early_sent.wait_send()
                late_sent.wait_send()
            remote(z_rx.at[par], z_rx.at[par], zs_sem.at[par], zr_sem.at[par, 0], z_peers[0]).wait_send()
    sent = x_v.at[pl.ds(own_rows, own_rows)]
    remote(sent, sent, xs_sem.at[0], xr_sem.at[0], c_peer).wait_send()


def store_kernel(mu_ref, lp_ref, lse_ref, mu_out, lp_out, lse_out, sems):
    copies = []
    parts = 4
    step = mu_ref.shape[1] // parts
    for s in range(mu_ref.shape[0]):
        for i in range(parts):
            rows = pl.ds(i * step, step)
            copies.append(
                pltpu.make_async_copy(mu_ref.at[s, rows], mu_out.at[s, rows], sems.at[2 + s * parts + i])
            )
    copies.append(pltpu.make_async_copy(lp_ref, lp_out, sems.at[0]))
    copies.append(pltpu.make_async_copy(lse_ref, lse_out, sems.at[1]))
    for cp in copies:
        cp.start()
    for cp in copies:
        cp.wait()


def solution(mesh):
    n_z = mesh.shape["comp"]
    row_size = mesh.shape["row"]

    def local_fit(x_local, mu_init, logpi_init, inv_temp):
        n_rows, full_dim = x_local.shape
        _, k_dim, h_dim = mu_init.shape
        n_sweeps = inv_temp.shape[0]
        total = 2 * n_rows
        chunk = total // N_CHUNKS
        k_half = k_dim // 2
        col_blocks = h_dim // 128
        log_denom = float(n_rows * row_size + k_dim * n_z * PRIOR_ALPHA)
        f32 = jnp.float32
        bf16 = jnp.bfloat16
        dma = pltpu.SemaphoreType.DMA
        mu, lp, lse = pl.pallas_call(
            functools.partial(em_kernel, n_z, n_sweeps, log_denom),
            out_shape=(
                pltpu.VMEM((2, k_dim, h_dim), f32),
                pltpu.VMEM((2, k_dim), f32),
                pltpu.VMEM((2, n_rows), f32),
            ),
            in_specs=[pl.BlockSpec(memory_space=pltpu.HBM)] * 4,
            out_specs=(
                pl.BlockSpec(memory_space=pltpu.VMEM),
                pl.BlockSpec(memory_space=pltpu.VMEM),
                pl.BlockSpec(memory_space=pltpu.VMEM),
            ),
            scratch_shapes=[
                pltpu.VMEM((total, h_dim), bf16),
                pltpu.VMEM((h_dim, total), bf16),
                pltpu.VMEM((k_dim, h_dim), f32),
                pltpu.VMEM((k_dim, h_dim), bf16),
                pltpu.VMEM((k_dim, total), f32),
                pltpu.VMEM((k_dim, total), bf16),
                pltpu.VMEM((k_dim, h_dim), f32),
                pltpu.VMEM((k_dim, h_dim), f32),
                pltpu.VMEM((2, 1, k_dim), f32),
                pltpu.VMEM((2, 1, k_dim), f32),
                pltpu.VMEM((2, 1, k_half), f32),
                pltpu.VMEM((2, 1, k_half), f32),
                pltpu.VMEM((2, N_CHUNKS, 1, chunk), f32),
                pltpu.VMEM((2, N_CHUNKS, n_z - 1, 1, chunk), f32),
                pltpu.VMEM((2, 1, total), f32),
                pltpu.VMEM((1, total), f32),
                pltpu.VMEM((1, total), f32),
                pltpu.VMEM((1, total), f32),
                pltpu.VMEM((1, n_rows), f32),
                pltpu.VMEM((1, k_dim), f32),
                pltpu.VMEM((2, k_dim), f32),
                pltpu.SMEM((n_sweeps,), f32),
                dma((3 + N_CHUNKS // 2,)),
                dma((1,)), dma((N_CHUNKS // 2,)),
                dma((2,)), dma((2, N_CHUNKS)),
                dma((2,)), dma((2 * col_blocks,)),
                dma((1,)), dma((1,)),
                dma((1,)), dma((1,)),
                dma((1,)), dma((1,)),
                dma((2,)), dma((2,)),
                dma((1,)), dma((1,)),
                pltpu.SemaphoreType.REGULAR,
            ],
            compiler_params=pltpu.CompilerParams(
                collective_id=0, has_side_effects=True, vmem_limit_bytes=VMEM_LIMIT
            ),
            name="em_kernel",
        )(*[pltpu.with_memory_space_constraint(v, pltpu.HBM) for v in (x_local, mu_init, logpi_init, inv_temp)])
        return pl.pallas_call(
            store_kernel,
            out_shape=(
                jax.ShapeDtypeStruct((2, k_dim, h_dim), f32),
                jax.ShapeDtypeStruct((2, k_dim), f32),
                jax.ShapeDtypeStruct((2, n_rows), f32),
            ),
            in_specs=[pl.BlockSpec(memory_space=pltpu.VMEM)] * 3,
            out_specs=(pl.BlockSpec(memory_space=pl.ANY),) * 3,
            scratch_shapes=[dma((2 + 2 * 4,))],
            compiler_params=pltpu.CompilerParams(vmem_limit_bytes=4 * 1024 * 1024),
            name="store_kernel",
        )(mu, lp, lse)

    return jax.shard_map(
        local_fit,
        mesh=mesh,
        in_specs=(P(("grp", "row"), None), P(None, ("grp", "comp"), None), P(None, ("grp", "comp")), P()),
        out_specs=(P(None, ("grp", "comp"), None), P(None, ("grp", "comp")), P(None, ("grp", "row"))),
        check_vma=False,
    )
```

```python
import functools

import jax
import jax.numpy as jnp
from jax import lax
from jax.experimental import pallas as pl
from jax.experimental.pallas import tpu as pltpu
from jax.sharding import PartitionSpec as P

EPS_COUNT = 1e-6
PRIOR_ALPHA = 1e-3
MESH = pl.DeviceIdType.MESH
LANE_BLOCK = 512
FIRST_TURN = 0
TURN_AT = 2
SWAP_SIZES = (1024, 512, 512)
LATER_SIZES = (1536, 1536, 1024)
VMEM_LIMIT = 40 * 1024 * 1024


def _col(row):
    n = row.shape[1]
    parts = [
        jnp.transpose(jnp.broadcast_to(row[:, i : i + 128], (128, 128)))
        for i in range(0, n, 128)
    ]
    return parts[0] if len(parts) == 1 else jnp.concatenate(parts, axis=0)


def _lane_sum_row(block):
    n = block.shape[0]
    parts = [
        jnp.sum(jnp.transpose(block[i : i + 128, :]), axis=0, keepdims=True)
        for i in range(0, n, 128)
    ]
    return parts[0] if len(parts) == 1 else jnp.concatenate(parts, axis=1)


def _fold(x):
    acc = x[:, 0:128]
    for i in range(128, x.shape[1], 128):
        acc = acc + x[:, i : i + 128]
    return acc


def em_kernel(
    n_z, n_sweeps, log_denom,
    x_hbm, mu_hbm, lp_hbm, beta_hbm,
    mu_out, lp_out, lse_out,
    x_v, x_o, x_t, mu_f, mu_b, p_v, r_v, s_v, s_rx, s_rx_end, n_tx, n_rx, c_tx, c_rx,
    z_tx, z_rx, m_v, l_v, sqx_v, lse_v, lse_rx, lp_rx, lp_v, beta_ref,
    ld_sem, xs_sem, xr_sem, zs_sem, zr_sem, ss_sem, sr_sem, ns_sem, nr_sem,
    as_sem, ar_sem, cs_sem, cr_sem, ls_sem, lr_sem, os_sem, or_sem, turn_sem,
):
    row = lax.axis_index("row")
    zz = lax.axis_index("comp")
    core = lax.rem(row, 2)
    yy = lax.div(row, 2)
    fit = lax.rem(core + yy, 2)
    other = 1 - fit
    y_peer = {"row": (1 - yy) * 2 + (1 - core)}
    c_peer = {"row": yy * 2 + (1 - core)}
    z_peers = [{"comp": lax.rem(zz + d, n_z)} for d in range(1, n_z)]

    n_rows = x_v.shape[0]
    own_rows = n_rows // 2
    k_dim, h_dim = mu_f.shape
    k_half = k_dim // 2
    mine = pl.multiple_of(yy * k_half, k_half)
    theirs = pl.multiple_of((1 - yy) * k_half, k_half)
    own_spans = [(i * own_rows // 2, own_rows // 2) for i in range(2)]
    swap_spans = []
    for size in SWAP_SIZES:
        swap_spans.append((sum(SWAP_SIZES[: len(swap_spans)]), size))
    first_spans = own_spans + [(own_rows + o, size) for o, size in swap_spans]
    later_spans = []
    for size in LATER_SIZES:
        later_spans.append((sum(LATER_SIZES[: len(later_spans)]), size))
    n_col = h_dim // 128
    col_blocks = [slice(g * 128, (g + 1) * 128) for g in range(n_col)]
    lanes = LANE_BLOCK // 128

    def remote(src, dst, send, recv, peer):
        return pltpu.make_async_remote_copy(
            src_ref=src, dst_ref=dst, send_sem=send, recv_sem=recv, device_id=peer, device_id_type=MESH
        )

    barrier = pltpu.get_barrier_semaphore()
    for peer in [c_peer, y_peer] + z_peers:
        pl.semaphore_signal(barrier, inc=1, device_id=peer, device_id_type=MESH)

    my_cols = pl.ds(pl.multiple_of(fit * h_dim, h_dim), h_dim)
    your_cols = pl.ds(pl.multiple_of(other * h_dim, h_dim), h_dim)
    beta_load = pltpu.make_async_copy(beta_hbm, beta_ref, ld_sem.at[0])
    lp_load = pltpu.make_async_copy(lp_hbm, lp_v, ld_sem.at[1])
    mu_load = pltpu.make_async_copy(mu_hbm.at[fit], mu_f, ld_sem.at[2])
    out_loads = []
    for i, (o, size) in enumerate(swap_spans):
        cp = pltpu.make_async_copy(x_hbm.at[pl.ds(o, size), your_cols], x_o.at[pl.ds(o, size)], ld_sem.at[5 + i])
        cp.start()
        out_loads.append(cp)
    for cp in (beta_load, lp_load, mu_load):
        cp.start()
    loads = []
    for i, (o, size) in enumerate(own_spans):
        cp = pltpu.make_async_copy(x_hbm.at[pl.ds(o, size), my_cols], x_v.at[pl.ds(o, size)], ld_sem.at[3 + i])
        cp.start()
        loads.append(cp)

    with jax.named_scope("enter"):
        pl.semaphore_wait(barrier, 1 + n_z)

    swaps = []
    for i, (o, size) in enumerate(swap_spans):
        out_loads[i].wait()
        cp = remote(x_o.at[pl.ds(o, size)], x_v.at[pl.ds(own_rows + o, size)], xs_sem.at[0], xr_sem.at[i], c_peer)
        cp.start()
        swaps.append(cp)

    with jax.named_scope("init"):
        beta_load.wait()
        lp_load.wait()
        mu_load.wait()
        mu0 = mu_f[...]
        mu_b[...] = mu0.astype(jnp.bfloat16)
        lp0 = jnp.where(fit == 0, lp_v[0:1, :], lp_v[1:2, :])
        c_row = lp0 - beta_ref[0] * _lane_sum_row(_fold(mu0 * mu0))
        c_col = _col(c_row)

    def softmax_half(lg, half, base, cols):
        m = jnp.max(lg, axis=0, keepdims=True)
        p = jnp.exp(lg - m)
        p_v[pl.ds(base, k_half), cols] = p
        m_v[half, :, cols] = m
        return m + jnp.log(jnp.sum(p, axis=0, keepdims=True))

    def log_add(u, v):
        top = jnp.maximum(u, v)
        return top + jnp.log(jnp.exp(u - top) + jnp.exp(v - top))

    def half_logits(base, cc, beta, cols):
        a = jnp.dot(mu_b[pl.ds(base, k_half), :], x_t[:, cols], preferred_element_type=jnp.float32)
        return a * (2.0 * beta) + jnp.concatenate([cc] * lanes, axis=1)

    for t in range(n_sweeps):
        last = t == n_sweeps - 1
        beta = beta_ref[t]
        par = t % 2
        spans = first_spans if t == 0 else later_spans
        for ci, (start, size) in enumerate(spans):
            if t == 0:
                with jax.named_scope("xwait"):
                    if ci < len(own_spans):
                        loads[ci].wait()
                    else:
                        swaps[ci - len(own_spans)].wait_recv()
            with jax.named_scope("estep"):
                for r0 in range(start, start + size, LANE_BLOCK):
                    cols = slice(r0, r0 + LANE_BLOCK)
                    if t == 0:
                        a = lax.dot_general(
                            mu_b[...], x_v[cols, :], (((1,), (1,)), ((), ())), preferred_element_type=jnp.float32
                        )
                        lg = a * (2.0 * beta) + jnp.concatenate([c_col] * lanes, axis=1)
                        l0 = softmax_half(lg[0:k_half, :], 0, 0, cols)
                        l1 = softmax_half(lg[k_half:, :], 1, k_half, cols)
                    else:
                        l0 = l_v[:, cols]
                        l1 = softmax_half(half_logits(theirs, c_their_col, beta, cols), 1 - yy, theirs, cols)
                    z_tx[par, :, cols] = log_add(l0, l1)
            span = pl.ds(start, size)
            for d, peer in enumerate(z_peers):
                remote(
                    z_tx.at[par, :, span], z_rx.at[par, d, :, span], zs_sem.at[par], zr_sem.at[par, ci], peer
                ).start()

        n_acc = jnp.zeros((k_dim, 128), jnp.float32)
        for ci, (start, size) in enumerate(spans):
            with jax.named_scope("zwait"):
                came = z_rx.at[par, :, :, pl.ds(start, size)]
                remote(came, came, zs_sem.at[par], zr_sem.at[par, ci], z_peers[0]).wait_recv()
            with jax.named_scope("resp"):
                for r0 in range(start, start + size, LANE_BLOCK):
                    cols = slice(r0, r0 + LANE_BLOCK)
                    parts = [z_tx[par, :, cols]] + [z_rx[par, d, :, cols] for d in range(n_z - 1)]
                    top = functools.reduce(jnp.maximum, parts)
                    tot = functools.reduce(lambda u, v: u + v, [jnp.exp(q - top) for q in parts])
                    lse = top + jnp.log(tot)
                    halves = []
                    for h in range(2):
                        ks = slice(h * k_half, (h + 1) * k_half)
                        r = p_v[ks, cols] * jnp.exp(m_v[h, :, cols] - lse)
                        r_v[ks, cols] = r.astype(jnp.bfloat16)
                        halves.append(_fold(r))
                    n_acc = n_acc + jnp.concatenate(halves, axis=0)
                    if last:
                        lse_v[:, cols] = lse - beta * sqx_v[:, cols]
                rows = slice(start, start + size)
                part = jnp.dot(r_v[pl.ds(theirs, k_half), rows], x_v[rows, :], preferred_element_type=jnp.float32)
                s_v[pl.ds(theirs, k_half), :] = part if ci == 0 else s_v[pl.ds(theirs, k_half), :] + part

        n_part = _lane_sum_row(n_acc)
        n_tx[par] = n_part
        n_copy = remote(n_tx.at[par], n_rx.at[par], ns_sem.at[0], nr_sem.at[0], y_peer)
        n_copy.start()

        def arrived(half, g):
            if g < n_col - 1:
                return s_rx.at[pl.ds(half, k_half), col_blocks[g]]
            return s_rx_end.at[par, pl.ds(half, k_half), :]

        def s_copy(half, g, second):
            end = g == n_col - 1
            slot = 2 * (n_col - 1) + 2 * par + second if end else second * (n_col - 1) + g
            return remote(
                s_v.at[pl.ds(half, k_half), col_blocks[g]], arrived(half, g),
                ss_sem.at[1 if end else 0], sr_sem.at[slot], y_peer,
            )

        first_copies = [s_copy(theirs, g, 0) for g in range(n_col)]
        s_mine = jax.named_scope("smine")
        early = s_v.at[pl.ds(theirs, k_half), pl.ds(0, h_dim - 128)]
        late = s_v.at[:, pl.ds(h_dim - 128, 128)]
        early_sent = remote(early, early, ss_sem.at[0], sr_sem.at[0], y_peer)
        late_sent = remote(late, late, ss_sem.at[1], sr_sem.at[0], y_peer)

        if t > 0:
            for cp in first_copies:
                cp.start()
        else:
            @pl.when(fit == FIRST_TURN)
            def _():
                for cp in first_copies:
                    cp.start()

        with s_mine:
            s_v[pl.ds(mine, k_half), :] = jnp.dot(
                r_v[pl.ds(mine, k_half), :], x_v[...], preferred_element_type=jnp.float32
            )
        last_copies = [s_copy(mine, g, 1) for g in (range(n_col) if last else [n_col - 1])]
        for cp in last_copies:
            cp.start()

        if t == 0:
            with jax.named_scope("xt"):
                for b in range(n_rows // LANE_BLOCK):
                    rows = slice(b * LANE_BLOCK, (b + 1) * LANE_BLOCK)
                    x_t[:, rows] = jnp.transpose(x_v[rows, :])
            with jax.named_scope("turn"):
                @pl.when(fit == 1 - FIRST_TURN)
                def _():
                    pl.semaphore_wait(turn_sem, 1)
                    for cp in first_copies:
                        cp.start()

            with jax.named_scope("sqx"):
                for b in range(n_rows // LANE_BLOCK):
                    cols = slice(b * LANE_BLOCK, (b + 1) * LANE_BLOCK)
                    xf = x_t[:, cols].astype(jnp.float32)
                    sqx_v[:, cols] = jnp.sum(xf * xf, axis=0, keepdims=True)

        with jax.named_scope("nwait"):
            n_copy.wait_recv()
        n_all = n_part + n_rx[par]
        if not last:
            n_own = jnp.where(yy == 0, n_all[:, 0:k_half], n_all[:, k_half:])
            n_their = jnp.where(yy == 0, n_all[:, k_half:], n_all[:, 0:k_half])
            inv_col = _col(1.0 / (n_own + EPS_COUNT))
            inv_their_col = _col(1.0 / (n_their + EPS_COUNT))
            beta_next = beta_ref[t + 1]

            def new_means(base, g, inv):
                cols = col_blocks[g]
                mu = (s_v[pl.ds(base, k_half), cols] + arrived(base, g)[...]) * inv
                mu_b[pl.ds(base, k_half), cols] = mu.astype(jnp.bfloat16)
                return mu * mu

            sq_acc = jnp.zeros((k_half, 128), jnp.float32)
            for g, cols in enumerate(col_blocks[:-1]):
                with jax.named_scope("ywait"):
                    first_copies[g].wait_recv()
                with jax.named_scope("mu"):
                    sq_acc = sq_acc + new_means(mine, g, inv_col)
                block = mu_b.at[pl.ds(mine, k_half), cols]
                remote(block, block, as_sem.at[0], ar_sem.at[0], y_peer).start()
                if t == 0 and g == TURN_AT:
                    @pl.when(fit == FIRST_TURN)
                    def _():
                        pl.semaphore_signal(turn_sem, inc=1, device_id=c_peer, device_id_type=MESH)
            c_part = jnp.log((n_own + PRIOR_ALPHA) / log_denom) - beta_next * _lane_sum_row(sq_acc)
            c_tx[par] = c_part
            c_copy = remote(c_tx.at[par], c_rx.at[par], cs_sem.at[0], cr_sem.at[0], y_peer)
            c_copy.start()
            with jax.named_scope("ywait"):
                first_copies[-1].wait_recv()
            c_own = c_part - beta_next * _lane_sum_row(new_means(mine, n_col - 1, inv_col))
            c_own_col = _col(c_own)
            with jax.named_scope("emine"):
                for b in range(n_rows // LANE_BLOCK):
                    cols = slice(b * LANE_BLOCK, (b + 1) * LANE_BLOCK)
                    l_v[:, cols] = softmax_half(
                        half_logits(mine, c_own_col, beta_next, cols), yy, mine, cols
                    )
            with jax.named_scope("cwait"):
                last_copies[0].wait_recv()
                sq_their = _lane_sum_row(new_means(theirs, n_col - 1, inv_their_col))
                c_copy.wait_recv()
                c_their_col = _col(c_rx[par] - beta_next * sq_their)
            with jax.named_scope("muwait"):
                rest = pl.ds(0, h_dim - 128)
                sent, came = mu_b.at[pl.ds(mine, k_half), rest], mu_b.at[pl.ds(theirs, k_half), rest]
                remote(sent, came, as_sem.at[0], ar_sem.at[0], y_peer).wait()
                c_copy.wait_send()
        else:
            lse_copy = remote(lse_v.at[:, pl.ds(own_rows, own_rows)], lse_rx, ls_sem.at[0], lr_sem.at[0], c_peer)
            lse_copy.start()
            lp_row = jnp.log((n_all + PRIOR_ALPHA) / log_denom)
            n_tx[1 - par] = lp_row
            lp_copy = remote(n_tx.at[1 - par], lp_rx, ls_sem.at[1], lr_sem.at[1], c_peer)
            lp_copy.start()
            inv_col = _col(1.0 / (n_all + EPS_COUNT))
            for half in range(2):
                base = mine if half == 0 else theirs
                inv_half = jnp.where(yy == half, inv_col[0:k_half, :], inv_col[k_half:, :])
                for g, cols in enumerate(col_blocks):
                    with jax.named_scope("fwait"):
                        (first_copies if half == 0 else last_copies)[g].wait_recv()
                    with jax.named_scope("fmu"):
                        mu_out[fit, pl.ds(base, k_half), cols] = (
                            s_v[pl.ds(base, k_half), cols] + arrived(base, g)[...]
                        ) * inv_half
                    block = mu_out.at[fit, pl.ds(base, k_half), cols]
                    remote(block, block, os_sem.at[0], or_sem.at[0], c_peer).start()
            lse_copy.wait_recv()
            own_lse = lse_v[:, 0:own_rows]
            lse_out[0:1, :] = jnp.where(fit == 0, own_lse, lse_rx[...])
            lse_out[1:2, :] = jnp.where(fit == 0, lse_rx[...], own_lse)
            lp_copy.wait_recv()
            lp_out[0:1, :] = jnp.where(fit == 0, lp_row, lp_rx[...])
            lp_out[1:2, :] = jnp.where(fit == 0, lp_rx[...], lp_row)
            lse_copy.wait_send()
            lp_copy.wait_send()
            with jax.named_scope("owait"):
                remote(mu_out.at[fit], mu_out.at[fit], os_sem.at[0], or_sem.at[0], c_peer).wait()
        with jax.named_scope("tail"):
            n_copy.wait_send()
            if last:
                both = s_v.at[:, pl.ds(0, h_dim - 128)]
                remote(both, both, ss_sem.at[0], sr_sem.at[0], y_peer).wait_send()
                both = s_v.at[:, pl.ds(h_dim - 128, 128)]
                remote(both, both, ss_sem.at[1], sr_sem.at[0], y_peer).wait_send()
            else:
                early_sent.wait_send()
                late_sent.wait_send()
            remote(z_rx.at[par], z_rx.at[par], zs_sem.at[par], zr_sem.at[par, 0], z_peers[0]).wait_send()
    sent = x_v.at[pl.ds(own_rows, own_rows)]
    remote(sent, sent, xs_sem.at[0], xr_sem.at[0], c_peer).wait_send()


def store_kernel(mu_ref, lp_ref, lse_ref, mu_out, lp_out, lse_out, sems):
    copies = []
    parts = 4
    step = mu_ref.shape[1] // parts
    for s in range(mu_ref.shape[0]):
        for i in range(parts):
            rows = pl.ds(i * step, step)
            copies.append(
                pltpu.make_async_copy(mu_ref.at[s, rows], mu_out.at[s, rows], sems.at[2 + s * parts + i])
            )
    copies.append(pltpu.make_async_copy(lp_ref, lp_out, sems.at[0]))
    copies.append(pltpu.make_async_copy(lse_ref, lse_out, sems.at[1]))
    for cp in copies:
        cp.start()
    for cp in copies:
        cp.wait()


def solution(mesh):
    n_z = mesh.shape["comp"]
    row_size = mesh.shape["row"]

    def local_fit(x_local, mu_init, logpi_init, inv_temp):
        n_rows, full_dim = x_local.shape
        _, k_dim, h_dim = mu_init.shape
        n_sweeps = inv_temp.shape[0]
        total = 2 * n_rows
        k_half = k_dim // 2
        col_blocks = h_dim // 128
        log_denom = float(n_rows * row_size + k_dim * n_z * PRIOR_ALPHA)
        f32 = jnp.float32
        bf16 = jnp.bfloat16
        dma = pltpu.SemaphoreType.DMA
        mu, lp, lse = pl.pallas_call(
            functools.partial(em_kernel, n_z, n_sweeps, log_denom),
            out_shape=(
                pltpu.VMEM((2, k_dim, h_dim), f32),
                pltpu.VMEM((2, k_dim), f32),
                pltpu.VMEM((2, n_rows), f32),
            ),
            in_specs=[pl.BlockSpec(memory_space=pltpu.HBM)] * 4,
            out_specs=(
                pl.BlockSpec(memory_space=pltpu.VMEM),
                pl.BlockSpec(memory_space=pltpu.VMEM),
                pl.BlockSpec(memory_space=pltpu.VMEM),
            ),
            scratch_shapes=[
                pltpu.VMEM((total, h_dim), bf16),
                pltpu.VMEM((n_rows, h_dim), bf16),
                pltpu.VMEM((h_dim, total), bf16),
                pltpu.VMEM((k_dim, h_dim), f32),
                pltpu.VMEM((k_dim, h_dim), bf16),
                pltpu.VMEM((k_dim, total), f32),
                pltpu.VMEM((k_dim, total), bf16),
                pltpu.VMEM((k_dim, h_dim), f32),
                pltpu.VMEM((k_dim, h_dim - 128), f32),
                pltpu.VMEM((2, k_dim, 128), f32),
                pltpu.VMEM((2, 1, k_dim), f32),
                pltpu.VMEM((2, 1, k_dim), f32),
                pltpu.VMEM((2, 1, k_half), f32),
                pltpu.VMEM((2, 1, k_half), f32),
                pltpu.VMEM((2, 1, total), f32),
                pltpu.VMEM((2, n_z - 1, 1, total), f32),
                pltpu.VMEM((2, 1, total), f32),
                pltpu.VMEM((1, total), f32),
                pltpu.VMEM((1, total), f32),
                pltpu.VMEM((1, total), f32),
                pltpu.VMEM((1, n_rows), f32),
                pltpu.VMEM((1, k_dim), f32),
                pltpu.VMEM((2, k_dim), f32),
                pltpu.SMEM((n_sweeps,), f32),
                dma((5 + len(SWAP_SIZES),)),
                dma((1,)), dma((len(SWAP_SIZES),)),
                dma((2,)), dma((2, max(2 + len(SWAP_SIZES), len(LATER_SIZES)))),
                dma((2,)), dma((2 * col_blocks + 2,)),
                dma((1,)), dma((1,)),
                dma((1,)), dma((1,)),
                dma((1,)), dma((1,)),
                dma((2,)), dma((2,)),
                dma((1,)), dma((1,)),
                pltpu.SemaphoreType.REGULAR,
            ],
            compiler_params=pltpu.CompilerParams(
                collective_id=0, has_side_effects=True, vmem_limit_bytes=VMEM_LIMIT
            ),
            name="em_kernel",
        )(*[pltpu.with_memory_space_constraint(v, pltpu.HBM) for v in (x_local, mu_init, logpi_init, inv_temp)])
        return pl.pallas_call(
            store_kernel,
            out_shape=(
                jax.ShapeDtypeStruct((2, k_dim, h_dim), f32),
                jax.ShapeDtypeStruct((2, k_dim), f32),
                jax.ShapeDtypeStruct((2, n_rows), f32),
            ),
            in_specs=[pl.BlockSpec(memory_space=pltpu.VMEM)] * 3,
            out_specs=(pl.BlockSpec(memory_space=pl.ANY),) * 3,
            scratch_shapes=[dma((2 + 2 * 4,))],
            compiler_params=pltpu.CompilerParams(vmem_limit_bytes=4 * 1024 * 1024),
            name="store_kernel",
        )(mu, lp, lse)

    return jax.shard_map(
        local_fit,
        mesh=mesh,
        in_specs=(P(("grp", "row"), None), P(None, ("grp", "comp"), None), P(None, ("grp", "comp")), P()),
        out_specs=(P(None, ("grp", "comp"), None), P(None, ("grp", "comp")), P(None, ("grp", "row"))),
        check_vma=False,
    )
```

```python
import functools

import jax
import jax.numpy as jnp
from jax import lax
from jax.experimental import pallas as pl
from jax.experimental.pallas import tpu as pltpu
from jax.sharding import PartitionSpec as P

EPS_COUNT = 1e-6
PRIOR_ALPHA = 1e-3
MESH = pl.DeviceIdType.MESH
LANE_BLOCK = 512
FIRST_TURN = 0
TURN_AT = 2
OWN_SPLIT = 3072
SWAP_SIZES = (1024, 512, 512)
LATER_SIZES = (1536, 1536, 1024)
VMEM_LIMIT = 40 * 1024 * 1024


def _col(row):
    n = row.shape[1]
    parts = [
        jnp.transpose(jnp.broadcast_to(row[:, i : i + 128], (128, 128)))
        for i in range(0, n, 128)
    ]
    return parts[0] if len(parts) == 1 else jnp.concatenate(parts, axis=0)


def _lane_sum_row(block):
    n = block.shape[0]
    parts = [
        jnp.sum(jnp.transpose(block[i : i + 128, :]), axis=0, keepdims=True)
        for i in range(0, n, 128)
    ]
    return parts[0] if len(parts) == 1 else jnp.concatenate(parts, axis=1)


def _fold(x):
    acc = x[:, 0:128]
    for i in range(128, x.shape[1], 128):
        acc = acc + x[:, i : i + 128]
    return acc


def em_kernel(
    n_z, n_sweeps, log_denom,
    x_hbm, mu_hbm, lp_hbm, beta_hbm,
    mu_out, lp_out, lse_out,
    x_v, x_t, mu_f, mu_b, p_v, r_v, s_v, s_rx, s_rx_end, n_tx, n_rx, c_tx, c_rx,
    z_tx, z_rx, m_v, l_v, sqx_v, lse_v, lse_rx, lp_rx, lp_v, beta_ref,
    ld_sem, xs_sem, xr_sem, zs_sem, zr_sem, ss_sem, sr_sem, ns_sem, nr_sem,
    as_sem, ar_sem, cs_sem, cr_sem, ls_sem, lr_sem, os_sem, or_sem, turn_sem, here_sem, all_sem,
):
    row = lax.axis_index("row")
    zz = lax.axis_index("comp")
    core = lax.rem(row, 2)
    yy = lax.div(row, 2)
    fit = lax.rem(core + yy, 2)
    other = 1 - fit
    y_peer = {"row": (1 - yy) * 2 + (1 - core)}
    c_peer = {"row": yy * 2 + (1 - core)}
    far, near = 3 * ((3 - zz) // 2), 1 + zz % 2
    z_index = [far, 6 - zz - far - near, near]
    z_peers = [{"comp": z} for z in z_index]
    z_slots = [lax.rem(z - zz + n_z, n_z) - 1 for z in z_index]

    n_rows = x_v.shape[0]
    own_rows = n_rows // 2
    k_dim, h_dim = mu_f.shape
    k_half = k_dim // 2
    mine = pl.multiple_of(yy * k_half, k_half)
    theirs = pl.multiple_of((1 - yy) * k_half, k_half)
    own_spans = [(i * own_rows // 2, own_rows // 2) for i in range(2)]
    swap_spans = []
    for size in SWAP_SIZES:
        swap_spans.append((sum(SWAP_SIZES[: len(swap_spans)]), size))
    first_spans = own_spans + [(own_rows + o, size) for o, size in swap_spans]
    later_spans = []
    for size in LATER_SIZES:
        later_spans.append((sum(LATER_SIZES[: len(later_spans)]), size))
    n_col = h_dim // 128
    col_blocks = [slice(g * 128, (g + 1) * 128) for g in range(n_col)]
    lanes = LANE_BLOCK // 128

    def remote(src, dst, send, recv, peer):
        return pltpu.make_async_remote_copy(
            src_ref=src, dst_ref=dst, send_sem=send, recv_sem=recv, device_id=peer, device_id_type=MESH
        )

    barrier = pltpu.get_barrier_semaphore()

    def signal(sem, peer):
        pl.semaphore_signal(sem, inc=1, device_id=peer, device_id_type=MESH)

    @pl.when(core == 1)
    def _():
        signal(barrier, c_peer)

    my_cols = pl.ds(pl.multiple_of(fit * h_dim, h_dim), h_dim)
    your_cols = pl.ds(pl.multiple_of(other * h_dim, h_dim), h_dim)
    beta_load = pltpu.make_async_copy(beta_hbm, beta_ref, ld_sem.at[0])
    lp_load = pltpu.make_async_copy(lp_hbm, lp_v, ld_sem.at[1])
    mu_load = pltpu.make_async_copy(mu_hbm.at[fit], mu_f, ld_sem.at[2])
    for cp in (beta_load, lp_load, mu_load):
        cp.start()
    loads = []
    for i, (o, size) in enumerate(own_spans):
        cp = pltpu.make_async_copy(x_hbm.at[pl.ds(o, size), my_cols], x_v.at[pl.ds(o, size)], ld_sem.at[3 + i])
        cp.start()
        loads.append(cp)

    with jax.named_scope("enter"):
        @pl.when(core == 0)
        def _():
            pl.semaphore_wait(barrier, 1)
            signal(here_sem, c_peer)

        @pl.when(core == 1)
        def _():
            pl.semaphore_wait(here_sem, 1)
            for peer in [{"row": (1 - yy) * 2 + 1}] + z_peers:
                signal(barrier, peer)

    swaps = []
    for i, (o, size) in enumerate(swap_spans):
        cp = remote(x_hbm.at[pl.ds(o, size), your_cols], x_v.at[pl.ds(own_rows + o, size)], xs_sem.at[0], xr_sem.at[i], c_peer)
        cp.start()
        swaps.append(cp)

    with jax.named_scope("init"):
        beta_load.wait()
        lp_load.wait()
        mu_load.wait()
        mu0 = mu_f[...]
        mu_b[...] = mu0.astype(jnp.bfloat16)
        lp0 = jnp.where(fit == 0, lp_v[0:1, :], lp_v[1:2, :])
        c_row = lp0 - beta_ref[0] * _lane_sum_row(_fold(mu0 * mu0))
        c_col = _col(c_row)

    def softmax_half(lg, half, base, cols):
        m = jnp.max(lg, axis=0, keepdims=True)
        p = jnp.exp(lg - m)
        p_v[pl.ds(base, k_half), cols] = p
        m_v[half, :, cols] = m
        return m + jnp.log(jnp.sum(p, axis=0, keepdims=True))

    def log_add(u, v):
        top = jnp.maximum(u, v)
        return top + jnp.log(jnp.exp(u - top) + jnp.exp(v - top))

    def half_logits(base, cc, beta, cols):
        a = jnp.dot(mu_b[pl.ds(base, k_half), :], x_t[:, cols], preferred_element_type=jnp.float32)
        return a * (2.0 * beta) + jnp.concatenate([cc] * lanes, axis=1)

    for t in range(n_sweeps):
        last = t == n_sweeps - 1
        beta = beta_ref[t]
        par = t % 2
        spans = first_spans if t == 0 else later_spans
        for ci, (start, size) in enumerate(spans):
            if t == 0:
                with jax.named_scope("xwait"):
                    if ci < len(own_spans):
                        loads[ci].wait()
                    else:
                        swaps[ci - len(own_spans)].wait_recv()
            with jax.named_scope("estep"):
                for r0 in range(start, start + size, LANE_BLOCK):
                    cols = slice(r0, r0 + LANE_BLOCK)
                    if t == 0:
                        a = lax.dot_general(
                            mu_b[...], x_v[cols, :], (((1,), (1,)), ((), ())), preferred_element_type=jnp.float32
                        )
                        lg = a * (2.0 * beta) + jnp.concatenate([c_col] * lanes, axis=1)
                        l0 = softmax_half(lg[0:k_half, :], 0, 0, cols)
                        l1 = softmax_half(lg[k_half:, :], 1, k_half, cols)
                    else:
                        l0 = l_v[:, cols]
                        l1 = softmax_half(half_logits(theirs, c_their_col, beta, cols), 1 - yy, theirs, cols)
                    z_tx[par, :, cols] = log_add(l0, l1)
            if t == 0 and ci == 0:
                with jax.named_scope("peers"):
                    @pl.when(core == 1)
                    def _():
                        pl.semaphore_wait(barrier, n_z)
                        signal(all_sem, c_peer)

                    @pl.when(core == 0)
                    def _():
                        pl.semaphore_wait(all_sem, 1)

            span = pl.ds(start, size)
            for slot, peer in zip(z_slots, z_peers):
                remote(
                    z_tx.at[par, :, span], z_rx.at[par, slot, :, span], zs_sem.at[par], zr_sem.at[par, ci], peer
                ).start()

        n_acc = jnp.zeros((k_dim, 128), jnp.float32)
        for ci, (start, size) in enumerate(spans):
            with jax.named_scope("zwait"):
                came = z_rx.at[par, :, :, pl.ds(start, size)]
                remote(came, came, zs_sem.at[par], zr_sem.at[par, ci], z_peers[0]).wait_recv()
            with jax.named_scope("resp"):
                for r0 in range(start, start + size, LANE_BLOCK):
                    cols = slice(r0, r0 + LANE_BLOCK)
                    parts = [z_tx[par, :, cols]] + [z_rx[par, d, :, cols] for d in range(n_z - 1)]
                    top = functools.reduce(jnp.maximum, parts)
                    tot = functools.reduce(lambda u, v: u + v, [jnp.exp(q - top) for q in parts])
                    lse = top + jnp.log(tot)
                    halves = []
                    for h in range(2):
                        ks = slice(h * k_half, (h + 1) * k_half)
                        r = p_v[ks, cols] * jnp.exp(m_v[h, :, cols] - lse)
                        r_v[ks, cols] = r.astype(jnp.bfloat16)
                        halves.append(_fold(r))
                    n_acc = n_acc + jnp.concatenate(halves, axis=0)
                    if last:
                        lse_v[:, cols] = lse - beta * sqx_v[:, cols]
                rows = slice(start, start + size)
                part = jnp.dot(r_v[pl.ds(theirs, k_half), rows], x_v[rows, :], preferred_element_type=jnp.float32)
                s_v[pl.ds(theirs, k_half), :] = part if ci == 0 else s_v[pl.ds(theirs, k_half), :] + part

        n_part = _lane_sum_row(n_acc)
        n_tx[par] = n_part
        n_copy = remote(n_tx.at[par], n_rx.at[par], ns_sem.at[0], nr_sem.at[0], y_peer)
        n_copy.start()

        def arrived(half, g):
            if g < n_col - 1:
                return s_rx.at[pl.ds(half, k_half), col_blocks[g]]
            return s_rx_end.at[par, pl.ds(half, k_half), :]

        def s_copy(half, g, second):
            end = g == n_col - 1
            slot = 2 * (n_col - 1) + 2 * par + second if end else second * (n_col - 1) + g
            return remote(
                s_v.at[pl.ds(half, k_half), col_blocks[g]], arrived(half, g),
                ss_sem.at[1 if end else 0], sr_sem.at[slot], y_peer,
            )

        first_copies = [s_copy(theirs, g, 0) for g in range(n_col)]
        s_mine = jax.named_scope("smine")
        early = s_v.at[pl.ds(theirs, k_half), pl.ds(0, h_dim - 128)]
        late = s_v.at[:, pl.ds(h_dim - 128, 128)]
        early_sent = remote(early, early, ss_sem.at[0], sr_sem.at[0], y_peer)
        late_sent = remote(late, late, ss_sem.at[1], sr_sem.at[0], y_peer)

        if t > 0:
            for cp in first_copies:
                cp.start()
        else:
            @pl.when(fit == FIRST_TURN)
            def _():
                for cp in first_copies:
                    cp.start()

        with s_mine:
            s_v[pl.ds(mine, k_half), :] = jnp.dot(
                r_v[pl.ds(mine, k_half), :], x_v[...], preferred_element_type=jnp.float32
            )
        last_copies = [s_copy(mine, g, 1) for g in (range(n_col) if last else [n_col - 1])]
        for cp in last_copies:
            cp.start()

        if t == 0:
            with jax.named_scope("xt"):
                for b in range(n_rows // LANE_BLOCK):
                    rows = slice(b * LANE_BLOCK, (b + 1) * LANE_BLOCK)
                    x_t[:, rows] = jnp.transpose(x_v[rows, :])
            with jax.named_scope("turn"):
                @pl.when(fit == 1 - FIRST_TURN)
                def _():
                    pl.semaphore_wait(turn_sem, 1)
                    for cp in first_copies:
                        cp.start()

            with jax.named_scope("sqx"):
                for b in range(n_rows // LANE_BLOCK):
                    cols = slice(b * LANE_BLOCK, (b + 1) * LANE_BLOCK)
                    xf = x_t[:, cols].astype(jnp.float32)
                    sqx_v[:, cols] = jnp.sum(xf * xf, axis=0, keepdims=True)

        with jax.named_scope("nwait"):
            n_copy.wait_recv()
        n_all = n_part + n_rx[par]
        if not last:
            n_own = jnp.where(yy == 0, n_all[:, 0:k_half], n_all[:, k_half:])
            n_their = jnp.where(yy == 0, n_all[:, k_half:], n_all[:, 0:k_half])
            inv_col = _col(1.0 / (n_own + EPS_COUNT))
            inv_their_col = _col(1.0 / (n_their + EPS_COUNT))
            beta_next = beta_ref[t + 1]

            def new_means(base, g, inv):
                cols = col_blocks[g]
                mu = (s_v[pl.ds(base, k_half), cols] + arrived(base, g)[...]) * inv
                mu_b[pl.ds(base, k_half), cols] = mu.astype(jnp.bfloat16)
                return mu * mu

            sq_acc = jnp.zeros((k_half, 128), jnp.float32)
            for g, cols in enumerate(col_blocks[:-1]):
                with jax.named_scope("ywait"):
                    first_copies[g].wait_recv()
                with jax.named_scope("mu"):
                    sq_acc = sq_acc + new_means(mine, g, inv_col)
                block = mu_b.at[pl.ds(mine, k_half), cols]
                remote(block, block, as_sem.at[0], ar_sem.at[0], y_peer).start()
                if t == 0 and g == TURN_AT:
                    @pl.when(fit == FIRST_TURN)
                    def _():
                        pl.semaphore_signal(turn_sem, inc=1, device_id=c_peer, device_id_type=MESH)
            c_part = jnp.log((n_own + PRIOR_ALPHA) / log_denom) - beta_next * _lane_sum_row(sq_acc)
            c_tx[par] = c_part
            c_copy = remote(c_tx.at[par], c_rx.at[par], cs_sem.at[0], cr_sem.at[0], y_peer)
            c_copy.start()
            with jax.named_scope("ywait"):
                first_copies[-1].wait_recv()
            c_own = c_part - beta_next * _lane_sum_row(new_means(mine, n_col - 1, inv_col))
            c_own_col = _col(c_own)
            def own_logits(lo, hi):
                for r0 in range(lo, hi, LANE_BLOCK):
                    cols = slice(r0, r0 + LANE_BLOCK)
                    l_v[:, cols] = softmax_half(half_logits(mine, c_own_col, beta_next, cols), yy, mine, cols)

            with jax.named_scope("emine"):
                own_logits(0, OWN_SPLIT)
            with jax.named_scope("bwait"):
                last_copies[0].wait_recv()
            with jax.named_scope("emine"):
                sq_their = beta_next * _lane_sum_row(new_means(theirs, n_col - 1, inv_their_col))
                own_logits(OWN_SPLIT, n_rows)
            with jax.named_scope("cwait"):
                c_copy.wait_recv()
                c_their_col = _col(c_rx[par] - sq_their)
            with jax.named_scope("muwait"):
                rest = pl.ds(0, h_dim - 128)
                sent, came = mu_b.at[pl.ds(mine, k_half), rest], mu_b.at[pl.ds(theirs, k_half), rest]
                remote(sent, came, as_sem.at[0], ar_sem.at[0], y_peer).wait()
                c_copy.wait_send()
        else:
            lse_copy = remote(lse_v.at[:, pl.ds(own_rows, own_rows)], lse_rx, ls_sem.at[0], lr_sem.at[0], c_peer)
            lse_copy.start()
            lp_row = jnp.log((n_all + PRIOR_ALPHA) / log_denom)
            n_tx[1 - par] = lp_row
            lp_copy = remote(n_tx.at[1 - par], lp_rx, ls_sem.at[1], lr_sem.at[1], c_peer)
            lp_copy.start()
            inv_col = _col(1.0 / (n_all + EPS_COUNT))
            for half in range(2):
                base = mine if half == 0 else theirs
                inv_half = jnp.where(yy == half, inv_col[0:k_half, :], inv_col[k_half:, :])
                for g, cols in enumerate(col_blocks):
                    with jax.named_scope("fwait"):
                        (first_copies if half == 0 else last_copies)[g].wait_recv()
                    with jax.named_scope("fmu"):
                        mu_out[fit, pl.ds(base, k_half), cols] = (
                            s_v[pl.ds(base, k_half), cols] + arrived(base, g)[...]
                        ) * inv_half
                    block = mu_out.at[fit, pl.ds(base, k_half), cols]
                    remote(block, block, os_sem.at[0], or_sem.at[0], c_peer).start()
            lse_copy.wait_recv()
            own_lse = lse_v[:, 0:own_rows]
            lse_out[0:1, :] = jnp.where(fit == 0, own_lse, lse_rx[...])
            lse_out[1:2, :] = jnp.where(fit == 0, lse_rx[...], own_lse)
            lp_copy.wait_recv()
            lp_out[0:1, :] = jnp.where(fit == 0, lp_row, lp_rx[...])
            lp_out[1:2, :] = jnp.where(fit == 0, lp_rx[...], lp_row)
            lse_copy.wait_send()
            lp_copy.wait_send()
            with jax.named_scope("owait"):
                remote(mu_out.at[fit], mu_out.at[fit], os_sem.at[0], or_sem.at[0], c_peer).wait()
        with jax.named_scope("tail"):
            n_copy.wait_send()
            if last:
                both = s_v.at[:, pl.ds(0, h_dim - 128)]
                remote(both, both, ss_sem.at[0], sr_sem.at[0], y_peer).wait_send()
                both = s_v.at[:, pl.ds(h_dim - 128, 128)]
                remote(both, both, ss_sem.at[1], sr_sem.at[0], y_peer).wait_send()
            else:
                early_sent.wait_send()
                late_sent.wait_send()
            remote(z_rx.at[par], z_rx.at[par], zs_sem.at[par], zr_sem.at[par, 0], z_peers[0]).wait_send()
    sent = x_v.at[pl.ds(own_rows, own_rows)]
    remote(sent, sent, xs_sem.at[0], xr_sem.at[0], c_peer).wait_send()


def store_kernel(mu_ref, lp_ref, lse_ref, mu_out, lp_out, lse_out, sems):
    copies = []
    parts = 4
    step = mu_ref.shape[1] // parts
    for s in range(mu_ref.shape[0]):
        for i in range(parts):
            rows = pl.ds(i * step, step)
            copies.append(
                pltpu.make_async_copy(mu_ref.at[s, rows], mu_out.at[s, rows], sems.at[2 + s * parts + i])
            )
    copies.append(pltpu.make_async_copy(lp_ref, lp_out, sems.at[0]))
    copies.append(pltpu.make_async_copy(lse_ref, lse_out, sems.at[1]))
    for cp in copies:
        cp.start()
    for cp in copies:
        cp.wait()


def solution(mesh):
    n_z = mesh.shape["comp"]
    row_size = mesh.shape["row"]

    def local_fit(x_local, mu_init, logpi_init, inv_temp):
        n_rows, full_dim = x_local.shape
        _, k_dim, h_dim = mu_init.shape
        n_sweeps = inv_temp.shape[0]
        total = 2 * n_rows
        k_half = k_dim // 2
        col_blocks = h_dim // 128
        log_denom = float(n_rows * row_size + k_dim * n_z * PRIOR_ALPHA)
        f32 = jnp.float32
        bf16 = jnp.bfloat16
        dma = pltpu.SemaphoreType.DMA
        mu, lp, lse = pl.pallas_call(
            functools.partial(em_kernel, n_z, n_sweeps, log_denom),
            out_shape=(
                pltpu.VMEM((2, k_dim, h_dim), f32),
                pltpu.VMEM((2, k_dim), f32),
                pltpu.VMEM((2, n_rows), f32),
            ),
            in_specs=[pl.BlockSpec(memory_space=pltpu.HBM)] * 4,
            out_specs=(
                pl.BlockSpec(memory_space=pltpu.VMEM),
                pl.BlockSpec(memory_space=pltpu.VMEM),
                pl.BlockSpec(memory_space=pltpu.VMEM),
            ),
            scratch_shapes=[
                pltpu.VMEM((total, h_dim), bf16),
                pltpu.VMEM((h_dim, total), bf16),
                pltpu.VMEM((k_dim, h_dim), f32),
                pltpu.VMEM((k_dim, h_dim), bf16),
                pltpu.VMEM((k_dim, total), f32),
                pltpu.VMEM((k_dim, total), bf16),
                pltpu.VMEM((k_dim, h_dim), f32),
                pltpu.VMEM((k_dim, h_dim - 128), f32),
                pltpu.VMEM((2, k_dim, 128), f32),
                pltpu.VMEM((2, 1, k_dim), f32),
                pltpu.VMEM((2, 1, k_dim), f32),
                pltpu.VMEM((2, 1, k_half), f32),
                pltpu.VMEM((2, 1, k_half), f32),
                pltpu.VMEM((2, 1, total), f32),
                pltpu.VMEM((2, n_z - 1, 1, total), f32),
                pltpu.VMEM((2, 1, total), f32),
                pltpu.VMEM((1, total), f32),
                pltpu.VMEM((1, total), f32),
                pltpu.VMEM((1, total), f32),
                pltpu.VMEM((1, n_rows), f32),
                pltpu.VMEM((1, k_dim), f32),
                pltpu.VMEM((2, k_dim), f32),
                pltpu.SMEM((n_sweeps,), f32),
                dma((5,)),
                dma((1,)), dma((len(SWAP_SIZES),)),
                dma((2,)), dma((2, max(2 + len(SWAP_SIZES), len(LATER_SIZES)))),
                dma((2,)), dma((2 * col_blocks + 2,)),
                dma((1,)), dma((1,)),
                dma((1,)), dma((1,)),
                dma((1,)), dma((1,)),
                dma((2,)), dma((2,)),
                dma((1,)), dma((1,)),
                pltpu.SemaphoreType.REGULAR,
                pltpu.SemaphoreType.REGULAR,
                pltpu.SemaphoreType.REGULAR,
            ],
            compiler_params=pltpu.CompilerParams(
                collective_id=0, has_side_effects=True, vmem_limit_bytes=VMEM_LIMIT
            ),
            name="em_kernel",
        )(*[pltpu.with_memory_space_constraint(v, pltpu.HBM) for v in (x_local, mu_init, logpi_init, inv_temp)])
        return pl.pallas_call(
            store_kernel,
            out_shape=(
                jax.ShapeDtypeStruct((2, k_dim, h_dim), f32),
                jax.ShapeDtypeStruct((2, k_dim), f32),
                jax.ShapeDtypeStruct((2, n_rows), f32),
            ),
            in_specs=[pl.BlockSpec(memory_space=pltpu.VMEM)] * 3,
            out_specs=(pl.BlockSpec(memory_space=pl.ANY),) * 3,
            scratch_shapes=[dma((2 + 2 * 4,))],
            compiler_params=pltpu.CompilerParams(vmem_limit_bytes=4 * 1024 * 1024),
            name="store_kernel",
        )(mu, lp, lse)

    return jax.shard_map(
        local_fit,
        mesh=mesh,
        in_specs=(P(("grp", "row"), None), P(None, ("grp", "comp"), None), P(None, ("grp", "comp")), P()),
        out_specs=(P(None, ("grp", "comp"), None), P(None, ("grp", "comp")), P(None, ("grp", "row"))),
        check_vma=False,
    )
```

```python
import functools

import jax
import jax.numpy as jnp
from jax import lax
from jax.experimental import pallas as pl
from jax.experimental.pallas import tpu as pltpu
from jax.sharding import PartitionSpec as P

EPS_COUNT = 1e-6
PRIOR_ALPHA = 1e-3
MESH = pl.DeviceIdType.MESH
LANE_BLOCK = 512
FIRST_TURN = 0
TURN_AT = 2
OWN_SPLIT = 3072
SWAP_SIZES = (1024, 512, 512)
LATER_SIZES = (1536, 1536, 1024)
VMEM_LIMIT = 40 * 1024 * 1024


def _col(row):
    n = row.shape[1]
    parts = [
        jnp.transpose(jnp.broadcast_to(row[:, i : i + 128], (128, 128)))
        for i in range(0, n, 128)
    ]
    return parts[0] if len(parts) == 1 else jnp.concatenate(parts, axis=0)


def _lane_sum_row(block):
    n = block.shape[0]
    parts = [
        jnp.sum(jnp.transpose(block[i : i + 128, :]), axis=0, keepdims=True)
        for i in range(0, n, 128)
    ]
    return parts[0] if len(parts) == 1 else jnp.concatenate(parts, axis=1)


def _fold(x):
    acc = x[:, 0:128]
    for i in range(128, x.shape[1], 128):
        acc = acc + x[:, i : i + 128]
    return acc


def em_kernel(
    n_z, n_sweeps, log_denom,
    x_hbm, mu_hbm, lp_hbm, beta_hbm,
    mu_out, lp_out, lse_out,
    x_v, x_t, mu_f, mu_b, p_v, r_v, s_v, s_rx, s_rx_end, n_tx, n_rx, c_tx, c_rx,
    z_tx, z_rx, m_v, l_v, sqx_v, lse_v, lse_rx, lp_rx, lp_v, beta_ref,
    ld_sem, xs_sem, xr_sem, zs_sem, zr_sem, ss_sem, sr_sem, ns_sem, nr_sem,
    as_sem, ar_sem, cs_sem, cr_sem, ls_sem, lr_sem, os_sem, or_sem, turn_sem, here_sem, all_sem,
):
    row = lax.axis_index("row")
    zz = lax.axis_index("comp")
    core = lax.rem(row, 2)
    yy = lax.div(row, 2)
    fit = lax.rem(core + yy, 2)
    other = 1 - fit
    y_peer = {"row": (1 - yy) * 2 + (1 - core)}
    c_peer = {"row": yy * 2 + (1 - core)}
    far, near = 3 * ((3 - zz) // 2), 1 + zz % 2
    z_index = [far, 6 - zz - far - near, near]
    z_peers = [{"comp": z} for z in z_index]
    z_slots = [lax.rem(z - zz + n_z, n_z) - 1 for z in z_index]

    n_rows = x_v.shape[0]
    own_rows = n_rows // 2
    k_dim, h_dim = mu_f.shape
    k_half = k_dim // 2
    mine = pl.multiple_of(yy * k_half, k_half)
    theirs = pl.multiple_of((1 - yy) * k_half, k_half)
    own_spans = [(i * own_rows // 2, own_rows // 2) for i in range(2)]
    swap_spans = []
    for size in SWAP_SIZES:
        swap_spans.append((sum(SWAP_SIZES[: len(swap_spans)]), size))
    first_spans = own_spans + [(own_rows + o, size) for o, size in swap_spans]
    later_spans = []
    for size in LATER_SIZES:
        later_spans.append((sum(LATER_SIZES[: len(later_spans)]), size))
    n_col = h_dim // 128
    col_blocks = [slice(g * 128, (g + 1) * 128) for g in range(n_col)]
    lanes = LANE_BLOCK // 128

    def remote(src, dst, send, recv, peer):
        return pltpu.make_async_remote_copy(
            src_ref=src, dst_ref=dst, send_sem=send, recv_sem=recv, device_id=peer, device_id_type=MESH
        )

    barrier = pltpu.get_barrier_semaphore()

    def signal(sem, peer):
        pl.semaphore_signal(sem, inc=1, device_id=peer, device_id_type=MESH)

    @pl.when(core == 1)
    def _():
        signal(barrier, c_peer)

    my_cols = pl.ds(pl.multiple_of(fit * h_dim, h_dim), h_dim)
    your_cols = pl.ds(pl.multiple_of(other * h_dim, h_dim), h_dim)
    beta_load = pltpu.make_async_copy(beta_hbm, beta_ref, ld_sem.at[0])
    lp_load = pltpu.make_async_copy(lp_hbm, lp_v, ld_sem.at[1])
    mu_load = pltpu.make_async_copy(mu_hbm.at[fit], mu_f, ld_sem.at[2])
    for cp in (beta_load, lp_load, mu_load):
        cp.start()
    loads = []
    for i, (o, size) in enumerate(own_spans):
        cp = pltpu.make_async_copy(x_hbm.at[pl.ds(o, size), my_cols], x_v.at[pl.ds(o, size)], ld_sem.at[3 + i])
        cp.start()
        loads.append(cp)

    with jax.named_scope("enter"):
        @pl.when(core == 0)
        def _():
            pl.semaphore_wait(barrier, 1)
            signal(here_sem, c_peer)

        @pl.when(core == 1)
        def _():
            pl.semaphore_wait(here_sem, 1)
            for peer in [{"row": (1 - yy) * 2 + 1}] + z_peers:
                signal(barrier, peer)

    swaps = []
    for i, (o, size) in enumerate(swap_spans):
        cp = remote(x_hbm.at[pl.ds(o, size), your_cols], x_v.at[pl.ds(own_rows + o, size)], xs_sem.at[0], xr_sem.at[i], c_peer)
        cp.start()
        swaps.append(cp)

    with jax.named_scope("init"):
        beta_load.wait()
        lp_load.wait()
        mu_load.wait()
        mu0 = mu_f[...]
        mu_b[...] = mu0.astype(jnp.bfloat16)
        lp0 = jnp.where(fit == 0, lp_v[0:1, :], lp_v[1:2, :])
        c_row = lp0 - beta_ref[0] * _lane_sum_row(_fold(mu0 * mu0))
        c_col = _col(c_row)

    def softmax_half(lg, half, base, cols):
        m = jnp.max(lg, axis=0, keepdims=True)
        p = jnp.exp(lg - m)
        p_v[pl.ds(base, k_half), cols] = p
        m_v[half, :, cols] = m
        return m + jnp.log(jnp.sum(p, axis=0, keepdims=True))

    def log_add(u, v):
        top = jnp.maximum(u, v)
        return top + jnp.log(jnp.exp(u - top) + jnp.exp(v - top))

    def half_logits(base, cc, beta, cols):
        points = jnp.concatenate([x_t[j] for j in range(cols.start // 128, cols.stop // 128)], axis=1)
        a = jnp.dot(mu_b[pl.ds(base, k_half), :], points, preferred_element_type=jnp.float32)
        return a * (2.0 * beta) + jnp.concatenate([cc] * lanes, axis=1)

    for t in range(n_sweeps):
        last = t == n_sweeps - 1
        beta = beta_ref[t]
        par = t % 2
        spans = first_spans if t == 0 else later_spans
        for ci, (start, size) in enumerate(spans):
            if t == 0:
                with jax.named_scope("xwait"):
                    if ci < len(own_spans):
                        loads[ci].wait()
                    else:
                        swaps[ci - len(own_spans)].wait_recv()
            with jax.named_scope("estep"):
                for r0 in range(start, start + size, LANE_BLOCK):
                    cols = slice(r0, r0 + LANE_BLOCK)
                    if t == 0:
                        a = lax.dot_general(
                            mu_b[...], x_v[cols, :], (((1,), (1,)), ((), ())), preferred_element_type=jnp.float32
                        )
                        lg = a * (2.0 * beta) + jnp.concatenate([c_col] * lanes, axis=1)
                        l0 = softmax_half(lg[0:k_half, :], 0, 0, cols)
                        l1 = softmax_half(lg[k_half:, :], 1, k_half, cols)
                    else:
                        l0 = l_v[:, cols]
                        l1 = softmax_half(half_logits(theirs, c_their_col, beta, cols), 1 - yy, theirs, cols)
                    z_tx[par, :, cols] = log_add(l0, l1)
            if t == 0 and ci == 0:
                with jax.named_scope("peers"):
                    @pl.when(core == 1)
                    def _():
                        pl.semaphore_wait(barrier, n_z)
                        signal(all_sem, c_peer)

                    @pl.when(core == 0)
                    def _():
                        pl.semaphore_wait(all_sem, 1)

            span = pl.ds(start, size)
            for slot, peer in zip(z_slots, z_peers):
                remote(
                    z_tx.at[par, :, span], z_rx.at[par, slot, :, span], zs_sem.at[par], zr_sem.at[par, ci], peer
                ).start()

        n_acc = jnp.zeros((k_dim, 128), jnp.float32)
        for ci, (start, size) in enumerate(spans):
            with jax.named_scope("zwait"):
                came = z_rx.at[par, :, :, pl.ds(start, size)]
                remote(came, came, zs_sem.at[par], zr_sem.at[par, ci], z_peers[0]).wait_recv()
            with jax.named_scope("resp"):
                for r0 in range(start, start + size, LANE_BLOCK):
                    cols = slice(r0, r0 + LANE_BLOCK)
                    parts = [z_tx[par, :, cols]] + [z_rx[par, d, :, cols] for d in range(n_z - 1)]
                    top = functools.reduce(jnp.maximum, parts)
                    tot = functools.reduce(lambda u, v: u + v, [jnp.exp(q - top) for q in parts])
                    lse = top + jnp.log(tot)
                    halves = []
                    for h in range(2):
                        ks = slice(h * k_half, (h + 1) * k_half)
                        r = p_v[ks, cols] * jnp.exp(m_v[h, :, cols] - lse)
                        r_v[ks, cols] = r.astype(jnp.bfloat16)
                        halves.append(_fold(r))
                    n_acc = n_acc + jnp.concatenate(halves, axis=0)
                    if last:
                        lse_v[:, cols] = lse - beta * sqx_v[:, cols]
                rows = slice(start, start + size)
                part = jnp.dot(r_v[pl.ds(theirs, k_half), rows], x_v[rows, :], preferred_element_type=jnp.float32)
                s_v[pl.ds(theirs, k_half), :] = part if ci == 0 else s_v[pl.ds(theirs, k_half), :] + part

        n_part = _lane_sum_row(n_acc)
        n_tx[par] = n_part
        n_copy = remote(n_tx.at[par], n_rx.at[par], ns_sem.at[0], nr_sem.at[0], y_peer)
        n_copy.start()

        def arrived(half, g):
            if g < n_col - 1:
                return s_rx.at[pl.ds(half, k_half), col_blocks[g]]
            return s_rx_end.at[par, pl.ds(half, k_half), :]

        def s_copy(half, g, second):
            end = g == n_col - 1
            slot = 2 * (n_col - 1) + 2 * par + second if end else second * (n_col - 1) + g
            return remote(
                s_v.at[pl.ds(half, k_half), col_blocks[g]], arrived(half, g),
                ss_sem.at[1 if end else 0], sr_sem.at[slot], y_peer,
            )

        first_copies = [s_copy(theirs, g, 0) for g in range(n_col)]
        s_mine = jax.named_scope("smine")
        early = s_v.at[pl.ds(theirs, k_half), pl.ds(0, h_dim - 128)]
        late = s_v.at[:, pl.ds(h_dim - 128, 128)]
        early_sent = remote(early, early, ss_sem.at[0], sr_sem.at[0], y_peer)
        late_sent = remote(late, late, ss_sem.at[1], sr_sem.at[0], y_peer)

        if t > 0:
            for cp in first_copies:
                cp.start()
        else:
            @pl.when(fit == FIRST_TURN)
            def _():
                for cp in first_copies:
                    cp.start()

        with s_mine:
            s_v[pl.ds(mine, k_half), :] = jnp.dot(
                r_v[pl.ds(mine, k_half), :], x_v[...], preferred_element_type=jnp.float32
            )
        last_copies = [s_copy(mine, g, 1) for g in (range(n_col) if last else [n_col - 1])]
        for cp in last_copies:
            cp.start()

        if t == 0:
            with jax.named_scope("xt"):
                for b in range(n_rows // LANE_BLOCK):
                    rows = slice(b * LANE_BLOCK, (b + 1) * LANE_BLOCK)
                    turned = jnp.transpose(x_v[rows, :])
                    for j in range(lanes):
                        x_t[b * lanes + j] = turned[:, j * 128 : (j + 1) * 128]
            with jax.named_scope("turn"):
                @pl.when(fit == 1 - FIRST_TURN)
                def _():
                    pl.semaphore_wait(turn_sem, 1)
                    for cp in first_copies:
                        cp.start()

            with jax.named_scope("sqx"):
                for j in range(n_rows // 128):
                    xf = x_t[j].astype(jnp.float32)
                    sqx_v[:, j * 128 : (j + 1) * 128] = jnp.sum(xf * xf, axis=0, keepdims=True)

        with jax.named_scope("nwait"):
            n_copy.wait_recv()
        n_all = n_part + n_rx[par]
        if not last:
            n_own = jnp.where(yy == 0, n_all[:, 0:k_half], n_all[:, k_half:])
            n_their = jnp.where(yy == 0, n_all[:, k_half:], n_all[:, 0:k_half])
            inv_col = _col(1.0 / (n_own + EPS_COUNT))
            inv_their_col = _col(1.0 / (n_their + EPS_COUNT))
            beta_next = beta_ref[t + 1]

            def new_means(base, g, inv):
                cols = col_blocks[g]
                mu = (s_v[pl.ds(base, k_half), cols] + arrived(base, g)[...]) * inv
                mu_b[pl.ds(base, k_half), cols] = mu.astype(jnp.bfloat16)
                return mu * mu

            sq_acc = jnp.zeros((k_half, 128), jnp.float32)
            for g, cols in enumerate(col_blocks[:-1]):
                with jax.named_scope("ywait"):
                    first_copies[g].wait_recv()
                with jax.named_scope("mu"):
                    sq_acc = sq_acc + new_means(mine, g, inv_col)
                block = mu_b.at[pl.ds(mine, k_half), cols]
                remote(block, block, as_sem.at[0], ar_sem.at[0], y_peer).start()
                if t == 0 and g == TURN_AT:
                    @pl.when(fit == FIRST_TURN)
                    def _():
                        pl.semaphore_signal(turn_sem, inc=1, device_id=c_peer, device_id_type=MESH)
            c_part = jnp.log((n_own + PRIOR_ALPHA) / log_denom) - beta_next * _lane_sum_row(sq_acc)
            c_tx[par] = c_part
            c_copy = remote(c_tx.at[par], c_rx.at[par], cs_sem.at[0], cr_sem.at[0], y_peer)
            c_copy.start()
            with jax.named_scope("ywait"):
                first_copies[-1].wait_recv()
            c_own = c_part - beta_next * _lane_sum_row(new_means(mine, n_col - 1, inv_col))
            c_own_col = _col(c_own)
            def own_logits(lo, hi):
                for r0 in range(lo, hi, LANE_BLOCK):
                    cols = slice(r0, r0 + LANE_BLOCK)
                    l_v[:, cols] = softmax_half(half_logits(mine, c_own_col, beta_next, cols), yy, mine, cols)

            with jax.named_scope("emine"):
                own_logits(0, OWN_SPLIT)
            with jax.named_scope("bwait"):
                last_copies[0].wait_recv()
            with jax.named_scope("emine"):
                sq_their = beta_next * _lane_sum_row(new_means(theirs, n_col - 1, inv_their_col))
                own_logits(OWN_SPLIT, n_rows)
            with jax.named_scope("cwait"):
                c_copy.wait_recv()
                c_their_col = _col(c_rx[par] - sq_their)
            with jax.named_scope("muwait"):
                rest = pl.ds(0, h_dim - 128)
                sent, came = mu_b.at[pl.ds(mine, k_half), rest], mu_b.at[pl.ds(theirs, k_half), rest]
                remote(sent, came, as_sem.at[0], ar_sem.at[0], y_peer).wait()
                c_copy.wait_send()
        else:
            lse_copy = remote(lse_v.at[:, pl.ds(own_rows, own_rows)], lse_rx, ls_sem.at[0], lr_sem.at[0], c_peer)
            lse_copy.start()
            lp_row = jnp.log((n_all + PRIOR_ALPHA) / log_denom)
            n_tx[1 - par] = lp_row
            lp_copy = remote(n_tx.at[1 - par], lp_rx, ls_sem.at[1], lr_sem.at[1], c_peer)
            lp_copy.start()
            inv_col = _col(1.0 / (n_all + EPS_COUNT))
            for half in range(2):
                base = mine if half == 0 else theirs
                inv_half = jnp.where(yy == half, inv_col[0:k_half, :], inv_col[k_half:, :])
                for g, cols in enumerate(col_blocks):
                    with jax.named_scope("fwait"):
                        (first_copies if half == 0 else last_copies)[g].wait_recv()
                    with jax.named_scope("fmu"):
                        mu_out[fit, pl.ds(base, k_half), cols] = (
                            s_v[pl.ds(base, k_half), cols] + arrived(base, g)[...]
                        ) * inv_half
                    block = mu_out.at[fit, pl.ds(base, k_half), cols]
                    remote(block, block, os_sem.at[0], or_sem.at[0], c_peer).start()
            lse_copy.wait_recv()
            own_lse = lse_v[:, 0:own_rows]
            lse_out[0:1, :] = jnp.where(fit == 0, own_lse, lse_rx[...])
            lse_out[1:2, :] = jnp.where(fit == 0, lse_rx[...], own_lse)
            lp_copy.wait_recv()
            lp_out[0:1, :] = jnp.where(fit == 0, lp_row, lp_rx[...])
            lp_out[1:2, :] = jnp.where(fit == 0, lp_rx[...], lp_row)
            lse_copy.wait_send()
            lp_copy.wait_send()
            with jax.named_scope("owait"):
                remote(mu_out.at[fit], mu_out.at[fit], os_sem.at[0], or_sem.at[0], c_peer).wait()
        with jax.named_scope("tail"):
            n_copy.wait_send()
            if last:
                both = s_v.at[:, pl.ds(0, h_dim - 128)]
                remote(both, both, ss_sem.at[0], sr_sem.at[0], y_peer).wait_send()
                both = s_v.at[:, pl.ds(h_dim - 128, 128)]
                remote(both, both, ss_sem.at[1], sr_sem.at[0], y_peer).wait_send()
            else:
                early_sent.wait_send()
                late_sent.wait_send()
            remote(z_rx.at[par], z_rx.at[par], zs_sem.at[par], zr_sem.at[par, 0], z_peers[0]).wait_send()
    sent = x_v.at[pl.ds(own_rows, own_rows)]
    remote(sent, sent, xs_sem.at[0], xr_sem.at[0], c_peer).wait_send()


def store_kernel(mu_ref, lp_ref, lse_ref, mu_out, lp_out, lse_out, sems):
    copies = []
    parts = 1
    step = mu_ref.shape[1] // parts
    for s in range(mu_ref.shape[0]):
        for i in range(parts):
            rows = pl.ds(i * step, step)
            copies.append(
                pltpu.make_async_copy(mu_ref.at[s, rows], mu_out.at[s, rows], sems.at[2 + s * parts + i])
            )
    copies.append(pltpu.make_async_copy(lp_ref, lp_out, sems.at[0]))
    copies.append(pltpu.make_async_copy(lse_ref, lse_out, sems.at[1]))
    for cp in copies:
        cp.start()
    for cp in copies:
        cp.wait()


def solution(mesh):
    n_z = mesh.shape["comp"]
    row_size = mesh.shape["row"]

    def local_fit(x_local, mu_init, logpi_init, inv_temp):
        n_rows, full_dim = x_local.shape
        _, k_dim, h_dim = mu_init.shape
        n_sweeps = inv_temp.shape[0]
        total = 2 * n_rows
        k_half = k_dim // 2
        col_blocks = h_dim // 128
        log_denom = float(n_rows * row_size + k_dim * n_z * PRIOR_ALPHA)
        f32 = jnp.float32
        bf16 = jnp.bfloat16
        dma = pltpu.SemaphoreType.DMA
        mu, lp, lse = pl.pallas_call(
            functools.partial(em_kernel, n_z, n_sweeps, log_denom),
            out_shape=(
                pltpu.VMEM((2, k_dim, h_dim), f32),
                pltpu.VMEM((2, k_dim), f32),
                pltpu.VMEM((2, n_rows), f32),
            ),
            in_specs=[pl.BlockSpec(memory_space=pltpu.HBM)] * 4,
            out_specs=(
                pl.BlockSpec(memory_space=pltpu.VMEM),
                pl.BlockSpec(memory_space=pltpu.VMEM),
                pl.BlockSpec(memory_space=pltpu.VMEM),
            ),
            scratch_shapes=[
                pltpu.VMEM((total, h_dim), bf16),
                pltpu.VMEM((total // 128, h_dim, 128), bf16),
                pltpu.VMEM((k_dim, h_dim), f32),
                pltpu.VMEM((k_dim, h_dim), bf16),
                pltpu.VMEM((k_dim, total), f32),
                pltpu.VMEM((k_dim, total), bf16),
                pltpu.VMEM((k_dim, h_dim), f32),
                pltpu.VMEM((k_dim, h_dim - 128), f32),
                pltpu.VMEM((2, k_dim, 128), f32),
                pltpu.VMEM((2, 1, k_dim), f32),
                pltpu.VMEM((2, 1, k_dim), f32),
                pltpu.VMEM((2, 1, k_half), f32),
                pltpu.VMEM((2, 1, k_half), f32),
                pltpu.VMEM((2, 1, total), f32),
                pltpu.VMEM((2, n_z - 1, 1, total), f32),
                pltpu.VMEM((2, 1, total), f32),
                pltpu.VMEM((1, total), f32),
                pltpu.VMEM((1, total), f32),
                pltpu.VMEM((1, total), f32),
                pltpu.VMEM((1, n_rows), f32),
                pltpu.VMEM((1, k_dim), f32),
                pltpu.VMEM((2, k_dim), f32),
                pltpu.SMEM((n_sweeps,), f32),
                dma((5,)),
                dma((1,)), dma((len(SWAP_SIZES),)),
                dma((2,)), dma((2, max(2 + len(SWAP_SIZES), len(LATER_SIZES)))),
                dma((2,)), dma((2 * col_blocks + 2,)),
                dma((1,)), dma((1,)),
                dma((1,)), dma((1,)),
                dma((1,)), dma((1,)),
                dma((2,)), dma((2,)),
                dma((1,)), dma((1,)),
                pltpu.SemaphoreType.REGULAR,
                pltpu.SemaphoreType.REGULAR,
                pltpu.SemaphoreType.REGULAR,
            ],
            compiler_params=pltpu.CompilerParams(
                collective_id=0, has_side_effects=True, vmem_limit_bytes=VMEM_LIMIT
            ),
            name="em_kernel",
        )(*[pltpu.with_memory_space_constraint(v, pltpu.HBM) for v in (x_local, mu_init, logpi_init, inv_temp)])
        return pl.pallas_call(
            store_kernel,
            out_shape=(
                jax.ShapeDtypeStruct((2, k_dim, h_dim), f32),
                jax.ShapeDtypeStruct((2, k_dim), f32),
                jax.ShapeDtypeStruct((2, n_rows), f32),
            ),
            in_specs=[pl.BlockSpec(memory_space=pltpu.VMEM)] * 3,
            out_specs=(pl.BlockSpec(memory_space=pl.ANY),) * 3,
            scratch_shapes=[dma((2 + 2 * 1,))],
            compiler_params=pltpu.CompilerParams(vmem_limit_bytes=4 * 1024 * 1024),
            name="store_kernel",
        )(mu, lp, lse)

    return jax.shard_map(
        local_fit,
        mesh=mesh,
        in_specs=(P(("grp", "row"), None), P(None, ("grp", "comp"), None), P(None, ("grp", "comp")), P()),
        out_specs=(P(None, ("grp", "comp"), None), P(None, ("grp", "comp")), P(None, ("grp", "row"))),
        check_vma=False,
    )
```

```python
import functools

import jax
import jax.numpy as jnp
from jax import lax
from jax.experimental import pallas as pl
from jax.experimental.pallas import tpu as pltpu
from jax.sharding import PartitionSpec as P

EPS_COUNT = 1e-6
PRIOR_ALPHA = 1e-3
MESH = pl.DeviceIdType.MESH
LANE_BLOCK = 512
FIRST_TURN = 0
TURN_AT = 2
OWN_SPLIT = 3072
SWAP_SIZES = (1024, 512, 512)
LATER_SIZES = (1536, 1536, 1024)
VMEM_LIMIT = 40 * 1024 * 1024


def _col(row):
    n = row.shape[1]
    parts = [
        jnp.transpose(jnp.broadcast_to(row[:, i : i + 128], (128, 128)))
        for i in range(0, n, 128)
    ]
    return parts[0] if len(parts) == 1 else jnp.concatenate(parts, axis=0)


def _lane_sum_row(block):
    n = block.shape[0]
    parts = [
        jnp.sum(jnp.transpose(block[i : i + 128, :]), axis=0, keepdims=True)
        for i in range(0, n, 128)
    ]
    return parts[0] if len(parts) == 1 else jnp.concatenate(parts, axis=1)


def _fold(x):
    acc = x[:, 0:128]
    for i in range(128, x.shape[1], 128):
        acc = acc + x[:, i : i + 128]
    return acc


def em_kernel(
    n_z, n_sweeps, log_denom,
    x_hbm, mu_hbm, lp_hbm, beta_hbm,
    mu_out, lp_out, lse_out,
    x_v, x_t, mu_f, mu_b, p_v, r_v, s_v, s_rx, s_rx_end, n_tx, n_rx, c_tx, c_rx,
    z_tx, z_rx, m_v, l_v, sqx_v, lse_v, lse_rx, lp_rx, lp_v, beta_ref,
    ld_sem, xs_sem, xr_sem, zs_sem, zr_sem, ss_sem, sr_sem, ns_sem, nr_sem,
    as_sem, ar_sem, cs_sem, cr_sem, ls_sem, lr_sem, os_sem, or_sem, turn_sem, here_sem, all_sem,
):
    row = lax.axis_index("row")
    zz = lax.axis_index("comp")
    core = lax.rem(row, 2)
    yy = lax.div(row, 2)
    fit = lax.rem(core + yy, 2)
    other = 1 - fit
    y_peer = {"row": (1 - yy) * 2 + (1 - core)}
    c_peer = {"row": yy * 2 + (1 - core)}
    far, near = 3 * ((3 - zz) // 2), 1 + zz % 2
    z_index = [far, 6 - zz - far - near, near]
    z_peers = [{"comp": z} for z in z_index]
    z_slots = [lax.rem(z - zz + n_z, n_z) - 1 for z in z_index]

    n_rows = x_v.shape[0]
    own_rows = n_rows // 2
    k_dim, h_dim = mu_f.shape
    k_half = k_dim // 2
    mine = pl.multiple_of(yy * k_half, k_half)
    theirs = pl.multiple_of((1 - yy) * k_half, k_half)
    own_spans = [(i * own_rows // 2, own_rows // 2) for i in range(2)]
    swap_spans = []
    for size in SWAP_SIZES:
        swap_spans.append((sum(SWAP_SIZES[: len(swap_spans)]), size))
    first_spans = own_spans + [(own_rows + o, size) for o, size in swap_spans]
    later_spans = []
    for size in LATER_SIZES:
        later_spans.append((sum(LATER_SIZES[: len(later_spans)]), size))
    n_col = h_dim // 128
    col_blocks = [slice(g * 128, (g + 1) * 128) for g in range(n_col)]
    lanes = LANE_BLOCK // 128

    def remote(src, dst, send, recv, peer):
        return pltpu.make_async_remote_copy(
            src_ref=src, dst_ref=dst, send_sem=send, recv_sem=recv, device_id=peer, device_id_type=MESH
        )

    barrier = pltpu.get_barrier_semaphore()

    def signal(sem, peer):
        pl.semaphore_signal(sem, inc=1, device_id=peer, device_id_type=MESH)

    @pl.when(core == 1)
    def _():
        signal(barrier, c_peer)

    my_cols = pl.ds(pl.multiple_of(fit * h_dim, h_dim), h_dim)
    your_cols = pl.ds(pl.multiple_of(other * h_dim, h_dim), h_dim)
    beta_load = pltpu.make_async_copy(beta_hbm, beta_ref, ld_sem.at[0])
    lp_load = pltpu.make_async_copy(lp_hbm, lp_v, ld_sem.at[1])
    mu_load = pltpu.make_async_copy(mu_hbm.at[fit], mu_f, ld_sem.at[2])
    for cp in (beta_load, lp_load, mu_load):
        cp.start()
    loads = []
    for i, (o, size) in enumerate(own_spans):
        cp = pltpu.make_async_copy(x_hbm.at[pl.ds(o, size), my_cols], x_v.at[pl.ds(o, size)], ld_sem.at[3 + i])
        cp.start()
        loads.append(cp)

    with jax.named_scope("enter"):
        @pl.when(core == 0)
        def _():
            pl.semaphore_wait(barrier, 1)
            signal(here_sem, c_peer)

        @pl.when(core == 1)
        def _():
            pl.semaphore_wait(here_sem, 1)
            for peer in [{"row": (1 - yy) * 2 + 1}] + z_peers:
                signal(barrier, peer)

    swaps = []
    for i, (o, size) in enumerate(swap_spans):
        cp = remote(x_hbm.at[pl.ds(o, size), your_cols], x_v.at[pl.ds(own_rows + o, size)], xs_sem.at[0], xr_sem.at[i], c_peer)
        cp.start()
        swaps.append(cp)

    with jax.named_scope("init"):
        beta_load.wait()
        lp_load.wait()
        mu_load.wait()
        mu0 = mu_f[...]
        mu_b[...] = mu0.astype(jnp.bfloat16)
        lp0 = jnp.where(fit == 0, lp_v[0:1, :], lp_v[1:2, :])
        c_row = lp0 - beta_ref[0] * _lane_sum_row(_fold(mu0 * mu0))
        c_col = _col(c_row)

    def softmax_half(lg, half, base, cols):
        m = jnp.max(lg, axis=0, keepdims=True)
        p = jnp.exp(lg - m)
        p_v[pl.ds(base, k_half), cols] = p
        m_v[half, :, cols] = m
        return m + jnp.log(jnp.sum(p, axis=0, keepdims=True))

    def log_add(u, v):
        top = jnp.maximum(u, v)
        return top + jnp.log(jnp.exp(u - top) + jnp.exp(v - top))

    def half_logits(base, cc, beta, cols):
        points = jnp.concatenate([x_t[j] for j in range(cols.start // 128, cols.stop // 128)], axis=1)
        a = jnp.dot(mu_b[pl.ds(base, k_half), :], points, preferred_element_type=jnp.float32)
        return a * (2.0 * beta) + jnp.concatenate([cc] * lanes, axis=1)

    for t in range(n_sweeps):
        last = t == n_sweeps - 1
        beta = beta_ref[t]
        par = t % 2
        spans = first_spans if t == 0 else later_spans
        for ci, (start, size) in enumerate(spans):
            if t == 0:
                with jax.named_scope("xwait"):
                    if ci < len(own_spans):
                        loads[ci].wait()
                    else:
                        swaps[ci - len(own_spans)].wait_recv()
            with jax.named_scope("estep"):
                for r0 in range(start, start + size, LANE_BLOCK):
                    cols = slice(r0, r0 + LANE_BLOCK)
                    if t == 0:
                        a = lax.dot_general(
                            mu_b[...], x_v[cols, :], (((1,), (1,)), ((), ())), preferred_element_type=jnp.float32
                        )
                        lg = a * (2.0 * beta) + jnp.concatenate([c_col] * lanes, axis=1)
                        l0 = softmax_half(lg[0:k_half, :], 0, 0, cols)
                        l1 = softmax_half(lg[k_half:, :], 1, k_half, cols)
                    else:
                        l0 = l_v[:, cols]
                        l1 = softmax_half(half_logits(theirs, c_their_col, beta, cols), 1 - yy, theirs, cols)
                    z_tx[par, :, cols] = log_add(l0, l1)
            if t == 0 and ci == 0:
                with jax.named_scope("peers"):
                    @pl.when(core == 1)
                    def _():
                        pl.semaphore_wait(barrier, n_z)
                        signal(all_sem, c_peer)

                    @pl.when(core == 0)
                    def _():
                        pl.semaphore_wait(all_sem, 1)

            span = pl.ds(start, size)
            for slot, peer in zip(z_slots, z_peers):
                remote(
                    z_tx.at[par, :, span], z_rx.at[par, slot, :, span], zs_sem.at[par], zr_sem.at[par * len(first_spans) + ci], peer
                ).start()

        n_acc = jnp.zeros((k_dim, 128), jnp.float32)
        for ci, (start, size) in enumerate(spans):
            with jax.named_scope("zwait"):
                came = z_rx.at[par, :, :, pl.ds(start, size)]
                remote(came, came, zs_sem.at[par], zr_sem.at[par * len(first_spans) + ci], z_peers[0]).wait_recv()
            with jax.named_scope("resp"):
                for r0 in range(start, start + size, LANE_BLOCK):
                    cols = slice(r0, r0 + LANE_BLOCK)
                    parts = [z_tx[par, :, cols]] + [z_rx[par, d, :, cols] for d in range(n_z - 1)]
                    top = functools.reduce(jnp.maximum, parts)
                    tot = functools.reduce(lambda u, v: u + v, [jnp.exp(q - top) for q in parts])
                    lse = top + jnp.log(tot)
                    halves = []
                    for h in range(2):
                        ks = slice(h * k_half, (h + 1) * k_half)
                        r = p_v[ks, cols] * jnp.exp(m_v[h, :, cols] - lse)
                        r_v[ks, cols] = r.astype(jnp.bfloat16)
                        halves.append(_fold(r))
                    n_acc = n_acc + jnp.concatenate(halves, axis=0)
                    if last:
                        lse_v[:, cols] = lse - beta * sqx_v[:, cols]
                rows = slice(start, start + size)
                part = jnp.dot(r_v[pl.ds(theirs, k_half), rows], x_v[rows, :], preferred_element_type=jnp.float32)
                s_v[pl.ds(theirs, k_half), :] = part if ci == 0 else s_v[pl.ds(theirs, k_half), :] + part

        n_part = _lane_sum_row(n_acc)
        n_tx[par] = n_part
        n_copy = remote(n_tx.at[par], n_rx.at[par], ns_sem.at[0], nr_sem.at[0], y_peer)
        n_copy.start()

        def arrived(half, g):
            if g < n_col - 1:
                return s_rx.at[pl.ds(half, k_half), col_blocks[g]]
            return s_rx_end.at[par, pl.ds(half, k_half), :]

        def s_copy(half, g, second):
            end = g == n_col - 1
            slot = 2 * (n_col - 1) + 2 * par + second if end else second * (n_col - 1) + g
            return remote(
                s_v.at[pl.ds(half, k_half), col_blocks[g]], arrived(half, g),
                ss_sem.at[1 if end else 0], sr_sem.at[slot], y_peer,
            )

        first_copies = [s_copy(theirs, g, 0) for g in range(n_col)]
        s_mine = jax.named_scope("smine")
        early = s_v.at[pl.ds(theirs, k_half), pl.ds(0, h_dim - 128)]
        late = s_v.at[:, pl.ds(h_dim - 128, 128)]
        early_sent = remote(early, early, ss_sem.at[0], sr_sem.at[0], y_peer)
        late_sent = remote(late, late, ss_sem.at[1], sr_sem.at[0], y_peer)

        if t > 0:
            for cp in first_copies:
                cp.start()
        else:
            @pl.when(fit == FIRST_TURN)
            def _():
                for cp in first_copies:
                    cp.start()

        with s_mine:
            s_v[pl.ds(mine, k_half), :] = jnp.dot(
                r_v[pl.ds(mine, k_half), :], x_v[...], preferred_element_type=jnp.float32
            )
        last_copies = [s_copy(mine, g, 1) for g in (range(n_col) if last else [n_col - 1])]
        for cp in last_copies:
            cp.start()

        if t == 0:
            with jax.named_scope("xt"):
                for b in range(n_rows // LANE_BLOCK):
                    rows = slice(b * LANE_BLOCK, (b + 1) * LANE_BLOCK)
                    turned = jnp.transpose(x_v[rows, :])
                    for j in range(lanes):
                        x_t[b * lanes + j] = turned[:, j * 128 : (j + 1) * 128]
            with jax.named_scope("turn"):
                @pl.when(fit == 1 - FIRST_TURN)
                def _():
                    pl.semaphore_wait(turn_sem, 1)
                    for cp in first_copies:
                        cp.start()

            with jax.named_scope("sqx"):
                for j in range(n_rows // 128):
                    xf = x_t[j].astype(jnp.float32)
                    sqx_v[:, j * 128 : (j + 1) * 128] = jnp.sum(xf * xf, axis=0, keepdims=True)

        with jax.named_scope("nwait"):
            n_copy.wait_recv()
        n_all = n_part + n_rx[par]
        if not last:
            n_own = jnp.where(yy == 0, n_all[:, 0:k_half], n_all[:, k_half:])
            n_their = jnp.where(yy == 0, n_all[:, k_half:], n_all[:, 0:k_half])
            inv_col = _col(1.0 / (n_own + EPS_COUNT))
            inv_their_col = _col(1.0 / (n_their + EPS_COUNT))
            beta_next = beta_ref[t + 1]

            def new_means(base, g, inv):
                cols = col_blocks[g]
                mu = (s_v[pl.ds(base, k_half), cols] + arrived(base, g)[...]) * inv
                mu_b[pl.ds(base, k_half), cols] = mu.astype(jnp.bfloat16)
                return mu * mu

            sq_acc = jnp.zeros((k_half, 128), jnp.float32)
            for g, cols in enumerate(col_blocks[:-1]):
                with jax.named_scope("ywait"):
                    first_copies[g].wait_recv()
                with jax.named_scope("mu"):
                    sq_acc = sq_acc + new_means(mine, g, inv_col)
                block = mu_b.at[pl.ds(mine, k_half), cols]
                remote(block, block, as_sem.at[0], ar_sem.at[0], y_peer).start()
                if t == 0 and g == TURN_AT:
                    @pl.when(fit == FIRST_TURN)
                    def _():
                        pl.semaphore_signal(turn_sem, inc=1, device_id=c_peer, device_id_type=MESH)
            c_part = jnp.log((n_own + PRIOR_ALPHA) / log_denom) - beta_next * _lane_sum_row(sq_acc)
            c_tx[par] = c_part
            c_copy = remote(c_tx.at[par], c_rx.at[par], cs_sem.at[0], cr_sem.at[0], y_peer)
            c_copy.start()
            with jax.named_scope("ywait"):
                first_copies[-1].wait_recv()
            c_own = c_part - beta_next * _lane_sum_row(new_means(mine, n_col - 1, inv_col))
            c_own_col = _col(c_own)
            def own_logits(lo, hi):
                for r0 in range(lo, hi, LANE_BLOCK):
                    cols = slice(r0, r0 + LANE_BLOCK)
                    l_v[:, cols] = softmax_half(half_logits(mine, c_own_col, beta_next, cols), yy, mine, cols)

            with jax.named_scope("emine"):
                own_logits(0, OWN_SPLIT)
            with jax.named_scope("bwait"):
                last_copies[0].wait_recv()
            with jax.named_scope("emine"):
                sq_their = beta_next * _lane_sum_row(new_means(theirs, n_col - 1, inv_their_col))
                own_logits(OWN_SPLIT, n_rows)
            with jax.named_scope("cwait"):
                c_copy.wait_recv()
                c_their_col = _col(c_rx[par] - sq_their)
            with jax.named_scope("muwait"):
                rest = pl.ds(0, h_dim - 128)
                sent, came = mu_b.at[pl.ds(mine, k_half), rest], mu_b.at[pl.ds(theirs, k_half), rest]
                remote(sent, came, as_sem.at[0], ar_sem.at[0], y_peer).wait()
                c_copy.wait_send()
        else:
            lse_copy = remote(lse_v.at[:, pl.ds(own_rows, own_rows)], lse_rx, ls_sem.at[0], lr_sem.at[0], c_peer)
            lse_copy.start()
            lp_row = jnp.log((n_all + PRIOR_ALPHA) / log_denom)
            n_tx[1 - par] = lp_row
            lp_copy = remote(n_tx.at[1 - par], lp_rx, ls_sem.at[1], lr_sem.at[1], c_peer)
            lp_copy.start()
            inv_col = _col(1.0 / (n_all + EPS_COUNT))
            for half in range(2):
                base = mine if half == 0 else theirs
                inv_half = jnp.where(yy == half, inv_col[0:k_half, :], inv_col[k_half:, :])
                for g, cols in enumerate(col_blocks):
                    with jax.named_scope("fwait"):
                        (first_copies if half == 0 else last_copies)[g].wait_recv()
                    with jax.named_scope("fmu"):
                        mu_out[fit, pl.ds(base, k_half), cols] = (
                            s_v[pl.ds(base, k_half), cols] + arrived(base, g)[...]
                        ) * inv_half
                    block = mu_out.at[fit, pl.ds(base, k_half), cols]
                    remote(block, block, os_sem.at[0], or_sem.at[0], c_peer).start()
            lse_copy.wait_recv()
            own_lse = lse_v[:, 0:own_rows]
            lse_out[0:1, :] = jnp.where(fit == 0, own_lse, lse_rx[...])
            lse_out[1:2, :] = jnp.where(fit == 0, lse_rx[...], own_lse)
            lp_copy.wait_recv()
            lp_out[0:1, :] = jnp.where(fit == 0, lp_row, lp_rx[...])
            lp_out[1:2, :] = jnp.where(fit == 0, lp_rx[...], lp_row)
            lse_copy.wait_send()
            lp_copy.wait_send()
            with jax.named_scope("owait"):
                remote(mu_out.at[fit], mu_out.at[fit], os_sem.at[0], or_sem.at[0], c_peer).wait()
        with jax.named_scope("tail"):
            n_copy.wait_send()
            if last:
                both = s_v.at[:, pl.ds(0, h_dim - 128)]
                remote(both, both, ss_sem.at[0], sr_sem.at[0], y_peer).wait_send()
                both = s_v.at[:, pl.ds(h_dim - 128, 128)]
                remote(both, both, ss_sem.at[1], sr_sem.at[0], y_peer).wait_send()
            else:
                early_sent.wait_send()
                late_sent.wait_send()
            remote(z_rx.at[par], z_rx.at[par], zs_sem.at[par], zr_sem.at[0], z_peers[0]).wait_send()
    sent = x_v.at[pl.ds(own_rows, own_rows)]
    remote(sent, sent, xs_sem.at[0], xr_sem.at[0], c_peer).wait_send()


def store_kernel(mu_ref, lp_ref, lse_ref, mu_out, lp_out, lse_out, sems):
    copies = []
    parts = 1
    step = mu_ref.shape[1] // parts
    for s in range(mu_ref.shape[0]):
        for i in range(parts):
            rows = pl.ds(i * step, step)
            copies.append(
                pltpu.make_async_copy(mu_ref.at[s, rows], mu_out.at[s, rows], sems.at[2 + s * parts + i])
            )
    copies.append(pltpu.make_async_copy(lp_ref, lp_out, sems.at[0]))
    copies.append(pltpu.make_async_copy(lse_ref, lse_out, sems.at[1]))
    for cp in copies:
        cp.start()
    for cp in copies:
        cp.wait()


def solution(mesh):
    n_z = mesh.shape["comp"]
    row_size = mesh.shape["row"]

    def local_fit(x_local, mu_init, logpi_init, inv_temp):
        n_rows, full_dim = x_local.shape
        _, k_dim, h_dim = mu_init.shape
        n_sweeps = inv_temp.shape[0]
        total = 2 * n_rows
        k_half = k_dim // 2
        col_blocks = h_dim // 128
        log_denom = float(n_rows * row_size + k_dim * n_z * PRIOR_ALPHA)
        f32 = jnp.float32
        bf16 = jnp.bfloat16
        dma = pltpu.SemaphoreType.DMA
        mu, lp, lse = pl.pallas_call(
            functools.partial(em_kernel, n_z, n_sweeps, log_denom),
            out_shape=(
                pltpu.VMEM((2, k_dim, h_dim), f32),
                pltpu.VMEM((2, k_dim), f32),
                pltpu.VMEM((2, n_rows), f32),
            ),
            in_specs=[pl.BlockSpec(memory_space=pltpu.HBM)] * 4,
            out_specs=(
                pl.BlockSpec(memory_space=pltpu.VMEM),
                pl.BlockSpec(memory_space=pltpu.VMEM),
                pl.BlockSpec(memory_space=pltpu.VMEM),
            ),
            scratch_shapes=[
                pltpu.VMEM((total, h_dim), bf16),
                pltpu.VMEM((total // 128, h_dim, 128), bf16),
                pltpu.VMEM((k_dim, h_dim), f32),
                pltpu.VMEM((k_dim, h_dim), bf16),
                pltpu.VMEM((k_dim, total), f32),
                pltpu.VMEM((k_dim, total), bf16),
                pltpu.VMEM((k_dim, h_dim), f32),
                pltpu.VMEM((k_dim, h_dim - 128), f32),
                pltpu.VMEM((2, k_dim, 128), f32),
                pltpu.VMEM((2, 1, k_dim), f32),
                pltpu.VMEM((2, 1, k_dim), f32),
                pltpu.VMEM((2, 1, k_half), f32),
                pltpu.VMEM((2, 1, k_half), f32),
                pltpu.VMEM((2, 1, total), f32),
                pltpu.VMEM((2, n_z - 1, 1, total), f32),
                pltpu.VMEM((2, 1, total), f32),
                pltpu.VMEM((1, total), f32),
                pltpu.VMEM((1, total), f32),
                pltpu.VMEM((1, total), f32),
                pltpu.VMEM((1, n_rows), f32),
                pltpu.VMEM((1, k_dim), f32),
                pltpu.VMEM((2, k_dim), f32),
                pltpu.SMEM((n_sweeps,), f32),
                dma((5,)),
                dma((1,)), dma((len(SWAP_SIZES),)),
                dma((2,)), dma((2 + len(SWAP_SIZES) + len(LATER_SIZES),)),
                dma((2,)), dma((2 * col_blocks + 2,)),
                dma((1,)), dma((1,)),
                dma((1,)), dma((1,)),
                dma((1,)), dma((1,)),
                dma((2,)), dma((2,)),
                dma((1,)), dma((1,)),
                pltpu.SemaphoreType.REGULAR,
                pltpu.SemaphoreType.REGULAR,
                pltpu.SemaphoreType.REGULAR,
            ],
            compiler_params=pltpu.CompilerParams(
                collective_id=0, has_side_effects=True, vmem_limit_bytes=VMEM_LIMIT
            ),
            name="em_kernel",
        )(*[pltpu.with_memory_space_constraint(v, pltpu.HBM) for v in (x_local, mu_init, logpi_init, inv_temp)])
        return pl.pallas_call(
            store_kernel,
            out_shape=(
                jax.ShapeDtypeStruct((2, k_dim, h_dim), f32),
                jax.ShapeDtypeStruct((2, k_dim), f32),
                jax.ShapeDtypeStruct((2, n_rows), f32),
            ),
            in_specs=[pl.BlockSpec(memory_space=pltpu.VMEM)] * 3,
            out_specs=(pl.BlockSpec(memory_space=pl.ANY),) * 3,
            scratch_shapes=[dma((2 + 2 * 1,))],
            compiler_params=pltpu.CompilerParams(vmem_limit_bytes=4 * 1024 * 1024),
            name="store_kernel",
        )(mu, lp, lse)

    return jax.shard_map(
        local_fit,
        mesh=mesh,
        in_specs=(P(("grp", "row"), None), P(None, ("grp", "comp"), None), P(None, ("grp", "comp")), P()),
        out_specs=(P(None, ("grp", "comp"), None), P(None, ("grp", "comp")), P(None, ("grp", "row"))),
        check_vma=False,
    )
```
